16 devices in a mesh: dp: 2 (over y, z), tp: 8 (over x, core).
Axes of the slice: x: 4, y: 2, z: 1, core: 2. Of those that a mesh axis runs over, the one named last changes fastest.
The devices are a block of a 4x4x8 slice.
Arguments:
- x_in: bfloat16 [32, 512, 3072], P('dp'), parts along dimension 0
- adapter_ids: int32 [32], P('dp'), parts along dimension 0
- gain_attn: float32 [3072], replicated
- gain_mlp: float32 [3072], replicated
- w_q: bfloat16 [3072, 32, 96], P(None, 'tp')
- w_k: bfloat16 [3072, 32, 96], P(None, 'tp')
- w_v: bfloat16 [3072, 32, 96], P(None, 'tp')
- w_o: bfloat16 [32, 96, 3072], P('tp')
- w_gate: bfloat16 [3072, 8192], P(None, 'tp')
- w_up: bfloat16 [3072, 8192], P(None, 'tp')
- w_down: bfloat16 [8192, 3072], P('tp')
- a_q: bfloat16 [16, 3072, 32], P(None, None, 'tp')
- b_q: bfloat16 [16, 32, 32, 96], P(None, None, 'tp')
- a_k: bfloat16 [16, 3072, 32], P(None, None, 'tp')
- b_k: bfloat16 [16, 32, 32, 96], P(None, None, 'tp')
- a_v: bfloat16 [16, 3072, 32], P(None, None, 'tp')
- b_v: bfloat16 [16, 32, 32, 96], P(None, None, 'tp')
- a_o: bfloat16 [16, 32, 96, 32], P(None, 'tp')
- b_o: bfloat16 [16, 32, 3072], P(None, None, 'tp')
- a_gate: bfloat16 [16, 3072, 32], P(None, None, 'tp')
- b_gate: bfloat16 [16, 32, 8192], P(None, None, 'tp')
- a_up: bfloat16 [16, 3072, 32], P(None, None, 'tp')
- b_up: bfloat16 [16, 32, 8192], P(None, None, 'tp')
- a_down: bfloat16 [16, 8192, 32], P(None, 'tp')
- b_down: bfloat16 [16, 32, 3072], P(None, None, 'tp')
Outputs:
- output: bfloat16 [32, 512, 3072], P('dp'), parts along dimension 0
There are 2 independent parts. The reference program is written for one: setup_inputs(seed, part) draws one part's arguments, and reference() takes and returns one part's arrays. A program takes and returns all parts, laid end to end along the dimension named above; an argument that names none is the same for every part.
All inputs are finite; a program needn't handle non-finite values.
Results may differ from the reference program's by a relative error of at most 0.02.
Values are sent between devices in bfloat16 or wider.
A program may use at most 768 MiB of HBM per device.

```python
import jax
import jax.numpy as jnp
from jax import lax

BATCH = 16
SEQ_LEN = 512
D_MODEL = 3072
HEADS = 32
KV_HEADS = 32
HEAD_DIM = 96
D_FF = 8192
RANK = 32
ADAPTERS = 16
LORA_ALPHA = 16
RMS_EPS = 1e-5
Q_WIDTH = HEADS * HEAD_DIM
KV_WIDTH = KV_HEADS * HEAD_DIM


def draw_normal(rng_key, arr_shape, w_std):
    return (jax.random.normal(rng_key, arr_shape, jnp.float32) * w_std).astype(jnp.bfloat16)


def lora_pair(rng_key, a_shape, b_shape, fan_in, w_gain):
    key_a, key_b = jax.random.split(rng_key)
    a_stack = draw_normal(key_a, a_shape, fan_in ** -0.5)
    b_stack = draw_normal(key_b, b_shape, 0.2 * w_gain * RANK ** 0.5 / LORA_ALPHA)
    return a_stack, b_stack


def draw_ids(rng_key):
    key_perm, key_fill, key_mix = jax.random.split(rng_key, 3)
    id_perm = jax.random.permutation(key_perm, ADAPTERS).astype(jnp.int32)
    id_fill = jax.random.randint(key_fill, (BATCH,), 0, ADAPTERS).astype(jnp.int32)
    id_all = jnp.concatenate([id_perm, id_fill])[:BATCH]
    return jax.random.permutation(key_mix, id_all).astype(jnp.int32)


def setup_inputs(seed: int = 0, part: int = 0) -> dict:
    root_key = jax.random.key(seed)
    key_x, key_ids = jax.random.split(jax.random.fold_in(root_key, part))
    shared_keys = jax.random.split(root_key, 16)
    x_in = (0.5 * jax.random.normal(key_x, (BATCH, SEQ_LEN, D_MODEL), jnp.float32)).astype(jnp.bfloat16)
    gain_attn = 1.0 + 0.2 * jax.random.normal(shared_keys[0], (D_MODEL,), jnp.float32)
    gain_mlp = 1.0 + 0.2 * jax.random.normal(shared_keys[1], (D_MODEL,), jnp.float32)
    w_q = draw_normal(shared_keys[2], (D_MODEL, HEADS, HEAD_DIM), 1.7 * D_MODEL ** -0.5)
    w_k = draw_normal(shared_keys[3], (D_MODEL, KV_HEADS, HEAD_DIM), 1.7 * D_MODEL ** -0.5)
    w_v = draw_normal(shared_keys[4], (D_MODEL, KV_HEADS, HEAD_DIM), D_MODEL ** -0.5)
    w_o = draw_normal(shared_keys[5], (HEADS, HEAD_DIM, D_MODEL), Q_WIDTH ** -0.5)
    w_gate = draw_normal(shared_keys[6], (D_MODEL, D_FF), D_MODEL ** -0.5)
    w_up = draw_normal(shared_keys[7], (D_MODEL, D_FF), D_MODEL ** -0.5)
    w_down = draw_normal(shared_keys[8], (D_FF, D_MODEL), D_FF ** -0.5)
    a_q, b_q = lora_pair(shared_keys[9], (ADAPTERS, D_MODEL, RANK), (ADAPTERS, RANK, HEADS, HEAD_DIM), D_MODEL, 1.7)
    a_k, b_k = lora_pair(shared_keys[10], (ADAPTERS, D_MODEL, RANK), (ADAPTERS, RANK, KV_HEADS, HEAD_DIM), D_MODEL, 1.7)
    a_v, b_v = lora_pair(shared_keys[11], (ADAPTERS, D_MODEL, RANK), (ADAPTERS, RANK, KV_HEADS, HEAD_DIM), D_MODEL, 1.0)
    a_o, b_o = lora_pair(shared_keys[12], (ADAPTERS, HEADS, HEAD_DIM, RANK), (ADAPTERS, RANK, D_MODEL), Q_WIDTH, 1.0)
    a_gate, b_gate = lora_pair(shared_keys[13], (ADAPTERS, D_MODEL, RANK), (ADAPTERS, RANK, D_FF), D_MODEL, 1.0)
    a_up, b_up = lora_pair(shared_keys[14], (ADAPTERS, D_MODEL, RANK), (ADAPTERS, RANK, D_FF), D_MODEL, 1.0)
    a_down, b_down = lora_pair(shared_keys[15], (ADAPTERS, D_FF, RANK), (ADAPTERS, RANK, D_MODEL), D_FF, 1.0)
    return dict(x_in=x_in, adapter_ids=draw_ids(key_ids), gain_attn=gain_attn, gain_mlp=gain_mlp,
                w_q=w_q, w_k=w_k, w_v=w_v, w_o=w_o, w_gate=w_gate, w_up=w_up, w_down=w_down,
                a_q=a_q, b_q=b_q, a_k=a_k, b_k=b_k, a_v=a_v, b_v=b_v, a_o=a_o, b_o=b_o,
                a_gate=a_gate, b_gate=b_gate, a_up=a_up, b_up=b_up, a_down=a_down, b_down=b_down)


def rms_scale(x_in, gain_vec):
    x_f32 = x_in.astype(jnp.float32)
    inv_rms = lax.rsqrt(jnp.mean(x_f32 * x_f32, axis=-1, keepdims=True) + RMS_EPS)
    return (x_f32 * inv_rms * gain_vec).astype(jnp.bfloat16)


def lora_proj(h_in, w_base, a_sel, b_sel):
    base_out = jnp.dot(h_in, w_base, preferred_element_type=jnp.float32)
    lora_mid = jnp.dot(h_in, a_sel, preferred_element_type=jnp.float32).astype(jnp.bfloat16)
    return base_out + (LORA_ALPHA / RANK) * jnp.dot(lora_mid, b_sel, preferred_element_type=jnp.float32)


def attend_head(head_item):
    q_head, k_head, v_head = head_item
    scores = jnp.dot(q_head, k_head.T, preferred_element_type=jnp.float32) * HEAD_DIM ** -0.5
    causal = jnp.arange(SEQ_LEN)[:, None] >= jnp.arange(SEQ_LEN)[None, :]
    prob_bf = jax.nn.softmax(jnp.where(causal, scores, -jnp.inf), axis=-1).astype(jnp.bfloat16)
    return jnp.dot(prob_bf, v_head, preferred_element_type=jnp.float32).astype(jnp.bfloat16)


def reference(x_in, adapter_ids, gain_attn, gain_mlp, w_q, w_k, w_v, w_o, w_gate, w_up, w_down,
              a_q, b_q, a_k, b_k, a_v, b_v, a_o, b_o, a_gate, b_gate, a_up, b_up, a_down, b_down):
    head_group = HEADS // KV_HEADS
    w_query = w_q.reshape(D_MODEL, Q_WIDTH)
    w_key = w_k.reshape(D_MODEL, KV_WIDTH)
    w_value = w_v.reshape(D_MODEL, KV_WIDTH)
    w_out = w_o.reshape(Q_WIDTH, D_MODEL)

    def one_sequence(seq_item):
        x_seq, adapter_id = seq_item
        h_norm = rms_scale(x_seq, gain_attn)
        q_all = lora_proj(h_norm, w_query, a_q[adapter_id], b_q[adapter_id].reshape(RANK, Q_WIDTH)).astype(jnp.bfloat16)
        k_all = lora_proj(h_norm, w_key, a_k[adapter_id], b_k[adapter_id].reshape(RANK, KV_WIDTH)).astype(jnp.bfloat16)
        v_all = lora_proj(h_norm, w_value, a_v[adapter_id], b_v[adapter_id].reshape(RANK, KV_WIDTH)).astype(jnp.bfloat16)
        q_heads = q_all.reshape(SEQ_LEN, HEADS, HEAD_DIM).transpose(1, 0, 2)
        k_heads = jnp.repeat(k_all.reshape(SEQ_LEN, KV_HEADS, HEAD_DIM).transpose(1, 0, 2), head_group, axis=0)
        v_heads = jnp.repeat(v_all.reshape(SEQ_LEN, KV_HEADS, HEAD_DIM).transpose(1, 0, 2), head_group, axis=0)
        att_heads = lax.map(attend_head, (q_heads, k_heads, v_heads))
        att_flat = att_heads.transpose(1, 0, 2).reshape(SEQ_LEN, Q_WIDTH)
        z_out = lora_proj(att_flat, w_out, a_o[adapter_id].reshape(Q_WIDTH, RANK), b_o[adapter_id])
        x_one = (x_seq.astype(jnp.float32) + z_out).astype(jnp.bfloat16)
        h_two = rms_scale(x_one, gain_mlp)
        z_gate = lora_proj(h_two, w_gate, a_gate[adapter_id], b_gate[adapter_id]).astype(jnp.bfloat16)
        z_up = lora_proj(h_two, w_up, a_up[adapter_id], b_up[adapter_id]).astype(jnp.bfloat16)
        mlp_mid = (jax.nn.silu(z_gate.astype(jnp.float32)) * z_up.astype(jnp.float32)).astype(jnp.bfloat16)
        z_down = lora_proj(mlp_mid, w_down, a_down[adapter_id], b_down[adapter_id])
        return (x_one.astype(jnp.float32) + z_down).astype(jnp.bfloat16)

    return lax.map(one_sequence, (x_in, adapter_ids))
```

```python
import functools
import math

import jax
import jax.numpy as jnp
from jax import lax
from jax.experimental import pallas as pl
from jax.experimental.pallas import tpu as pltpu
from jax.sharding import PartitionSpec as P

LORA_ALPHA = 16
RMS_EPS = 1e-5
CORES = 2
MESH = pl.DeviceIdType.MESH
F32, BF16 = jnp.float32, jnp.bfloat16
NT = (((1,), (1,)), ((), ()))
VMEM_LIMIT = 67_000_000


def dot(a, b):
    return jnp.dot(a, b, preferred_element_type=F32)


def dot_nt(a, b):
    return lax.dot_general(a, b, NT, preferred_element_type=F32)


def ring(n):
    me = lax.axis_index("tp")
    core, chip = lax.rem(me, CORES), lax.div(me, CORES)
    right = lax.rem(chip + 1, n) * CORES + core
    left = lax.rem(chip + n - 1, n) * CORES + core
    return core, chip, right, left, chip * CORES + 1 - core


def greet(*others):
    barrier = pltpu.get_barrier_semaphore()
    for other in others:
        pl.semaphore_signal(barrier, inc=1, device_id={"tp": other}, device_id_type=MESH)
    pl.semaphore_wait(barrier, len(others))


def remote(src, dst, send, recv, to):
    return pltpu.make_async_remote_copy(src_ref=src, dst_ref=dst, send_sem=send, recv_sem=recv, device_id={"tp": to},
                                        device_id_type=MESH)


def local(src, dst, sem):
    return pltpu.make_async_copy(src, dst, sem)


def rms_rows(src, dst, gain, rows, step):
    def chunk(k, carry):
        at = pl.ds(pl.multiple_of(k * step, step), step)
        v = src[at, :].astype(F32)
        inv = lax.rsqrt(jnp.mean(v * v, axis=-1, keepdims=True) + RMS_EPS)
        dst[at, :] = (v * inv * gain[...]).astype(BF16)
        return carry

    lax.fori_loop(0, rows // step, chunk, 0)


def head_windows(group, dim):
    out = []
    for h in range(group):
        lo, hi = h * dim, (h + 1) * dim
        start, stop = lo // 128 * 128, -(-hi // 128) * 128
        out.append((start, stop, lo - start, hi - start))
    return out


def attend(qkv, out, width, group, dim, qblock):
    seq = qkv.shape[0]
    lanes = group * dim

    def one_group(g, carry):
        base = pl.multiple_of(g * lanes, 128)
        for qb in range(seq // qblock):
            rows, keys = pl.ds(qb * qblock, qblock), (qb + 1) * qblock
            acc = [None] * (lanes // 128)
            mask = (lax.broadcasted_iota(jnp.int32, (qblock, keys), 0) + qb * qblock
                    >= lax.broadcasted_iota(jnp.int32, (qblock, keys), 1))
            for start, stop, lo, hi in head_windows(group, dim):
                size = stop - start
                lane_q = lax.broadcasted_iota(jnp.int32, (qblock, size), 1)
                lane_k = lax.broadcasted_iota(jnp.int32, (keys, size), 1)
                q = qkv[rows, pl.ds(base + start, size)]
                k = qkv[pl.ds(0, keys), pl.ds(width + base + start, size)]
                v = qkv[pl.ds(0, keys), pl.ds(2 * width + base + start, size)]
                q = jnp.where((lane_q >= lo) & (lane_q < hi), q, jnp.zeros_like(q))
                v = jnp.where((lane_k >= lo) & (lane_k < hi), v, jnp.zeros_like(v))
                scores = jnp.where(mask, dot_nt(q, k) * dim ** -0.5, -jnp.inf)
                top = jnp.max(scores, axis=-1, keepdims=True)
                e = jnp.exp(scores - top)
                prob = (e / jnp.sum(e, axis=-1, keepdims=True)).astype(BF16)
                o = dot(prob, v)
                for t in range(size // 128):
                    piece = o[:, t * 128:(t + 1) * 128]
                    j = start // 128 + t
                    acc[j] = piece if acc[j] is None else acc[j] + piece
            for j, piece in enumerate(acc):
                out[rows, pl.ds(base + j * 128, 128)] = piece.astype(BF16)
        return carry

    lax.fori_loop(0, width // lanes, one_group, 0)


def pick(shape, share, ranks, slots, axis):
    i = lax.broadcasted_iota(jnp.int32, shape, axis)
    t = lax.broadcasted_iota(jnp.int32, shape, 1 - axis)
    dev, slot, r = i // (slots * share), (i // share) % slots, i % share
    return jnp.where(t == slot * ranks + dev * share + r, 1.0, 0.0).astype(BF16)


def kernel_a(n, lag, keep, scale, group, dim, share,
             x, gain, wq, wk, wv, ar, bqkv, wide, agu, wo, wg, wu, wd, lml,
             att, ar_oth, b_oth, wide_f, agu_f, wo_f, wg_o, wu_o, wd_o, lml_o,
             wbuf, xbuf, hbuf, abuf, bbuf, qkv, attb, mids, sel,
             w_sem, x_sem, a_sem, bo_sem, bp_sem, d_send, d_recv, o_send, o_recv, m_send, m_recv,
             p_own, pr_send, pl_send, prl_recv, prr_recv, pfr_send, pfl_send, pfl_recv, pfr_recv, pp_send, pp_recv,
             r_send, l_send, own_sem, rl_recv, rr_recv, fr_send, fl_send, fl_recv, fr_recv):
    core, chip, right, left, partner = ring(n)
    before, after, opposite = lax.rem(chip + n - 1, n), lax.rem(chip + 1, n), lax.rem(chip + 2, n)
    across = opposite * CORES + core
    nseq, rows, own = x.shape[0] // CORES, x.shape[1], wq.shape[0]
    width = own * CORES
    first = core * nseq
    rank = bqkv.shape[1] // 3
    arows = ar.shape[1]
    crows = CORES * arows
    greet(right, left, partner, across)

    theirs, mine_at = pl.ds((1 - core) * nseq, nseq), pl.ds(first, nseq)
    near = [remote(ar.at[theirs], ar_oth, d_send.at[4], d_recv.at[4], partner)]
    near += [remote(w, wbuf.at[pl.ds(p * width + core * own, own)], d_send.at[p], d_recv.at[p], partner)
             for p, w in enumerate((wq, wk, wv))]
    near.append(remote(bqkv.at[theirs], b_oth, d_send.at[3], d_recv.at[3], partner))
    far = [remote(src, dst, o_send.at[k], o_recv.at[k], partner)
           for k, (src, dst) in enumerate(((lml.at[theirs], lml_o), (wg, wg_o), (wu, wu_o), (wd, wd_o)))]
    mine = [local(w, wbuf.at[pl.ds(p * width + core * own, own)], w_sem.at[p]) for p, w in enumerate((wq, wk, wv))]

    packs = [(wide, wide_f, True), (agu, agu_f, True), (wo, wo_f, False)]

    def pack_start(k):
        src, dst, _ = packs[k]
        remote(src, dst.at[chip, core], pr_send.at[k], prl_recv.at[k], right).start()
        remote(src, dst.at[chip, core], pl_send.at[k], prr_recv.at[k], left).start()
        local(src, dst.at[chip, core], p_own.at[k]).start()

    def pack_hops(k):
        src, dst, _ = packs[k]
        half = src.shape[0] // 2
        a, b = dst.at[before, core, pl.ds(0, half)], dst.at[after, core, pl.ds(half, half)]
        return remote(a, a, pfr_send.at[k], pfl_recv.at[k], right), remote(b, b, pfl_send.at[k], pfr_recv.at[k], left)

    def pack_pass(k):
        src, dst, _ = packs[k]
        hop_r, hop_l = pack_hops(k)
        remote(src, dst.at[before, core], pr_send.at[k], prl_recv.at[k], right).wait_recv()
        hop_r.start()
        remote(src, dst.at[after, core], pl_send.at[k], prr_recv.at[k], left).wait_recv()
        hop_l.start()

    def pack_push(k):
        src, dst, by_seq = packs[k]
        part = dst.at[:, core, theirs] if by_seq else dst.at[:, core]
        return remote(part, part, pp_send.at[k], pp_recv.at[k], partner)

    def pack_across(k):
        src, dst, _ = packs[k]
        half = src.shape[0] // 2
        local(src, dst.at[chip, core], p_own.at[k]).wait()
        a, b = dst.at[opposite, core, pl.ds(0, half)], dst.at[opposite, core, pl.ds(half, half)]
        remote(a, a, pfr_send.at[k], pfl_recv.at[k], right).wait_recv()
        remote(b, b, pfl_send.at[k], pfr_recv.at[k], left).wait_recv()
        pack_push(k).start()

    def pack_end(k):
        src, dst, by_seq = packs[k]
        remote(src, dst.at[chip, core], pr_send.at[k], prl_recv.at[k], right).wait_send()
        remote(src, dst.at[chip, core], pl_send.at[k], prr_recv.at[k], left).wait_send()
        for hop in pack_hops(k):
            hop.wait_send()
        pack_push(k).wait_send()
        part = dst.at[:, 1 - core, mine_at] if by_seq else dst.at[:, 1 - core]
        remote(part, part, pp_send.at[k], pp_recv.at[k], partner).wait_recv()

    def x_copy(g):
        return local(x.at[first + lax.rem(g, nseq)], xbuf.at[lax.rem(g, 2)], x_sem.at[lax.rem(g, 2)])

    def a_copies(s):
        slot = lax.rem(s, 2)
        own_at = pl.ds(pl.multiple_of(core * arows, arows), arows)
        oth_at = pl.ds(pl.multiple_of((1 - core) * arows, arows), arows)
        return [local(ar.at[first + s], abuf.at[slot, own_at], a_sem.at[slot, 0]),
                local(ar_oth.at[s], abuf.at[slot, oth_at], a_sem.at[slot, 1])]

    def b_copies(s):
        slot, out = lax.rem(s, 2), []
        for p in range(3):
            part = pl.ds(p * rank, rank)
            own_at = pl.ds(pl.multiple_of(core * own, 128), own)
            oth_at = pl.ds(pl.multiple_of((1 - core) * own, 128), own)
            out.append(local(bqkv.at[first + s, part], bbuf.at[slot, p, part, own_at], bo_sem.at[slot, p]))
            out.append(local(b_oth.at[s, part], bbuf.at[slot, p, part, oth_at], bp_sem.at[slot, p]))
        return out

    near[0].start()
    pack_start(0)
    for c in near[1:] + mine:
        c.start()
    x_copy(0).start()
    bbuf[...] = jnp.zeros_like(bbuf)
    sel[...] = pick(sel.shape, share, rank, arows // share, 1)
    near[0].wait()
    for c in a_copies(0):
        c.start()

    def rank_rows(j):
        return pl.ds(pl.multiple_of(j * crows, crows), crows)

    def mid_copies(s, source=None):
        froms = (chip, chip, chip) if source is None else source
        return [remote(mids.at[s, rank_rows(j)], mids.at[s, rank_rows(j)], m_send.at[k, s], m_recv.at[k, s], to)
                for k, (j, to) in enumerate(zip(froms, (right, left, across)))]

    def first_product(s, carry):
        slot = lax.rem(s, 2)
        x_copy(s + 1).start()

        @pl.when(s + 1 < nseq)
        def _():
            for c in a_copies(s + 1):
                c.start()

        @pl.when(s == nseq // 2)
        def _():
            pack_start(1)

        x_copy(s).wait()
        rms_rows(xbuf.at[slot], hbuf, gain, rows, 32)
        for c in a_copies(s):
            c.wait()
        mids[s, rank_rows(chip), :] = dot_nt(abuf[slot], hbuf[...]).astype(BF16)
        for c in mid_copies(s):
            c.start()
        return carry

    lax.fori_loop(0, nseq, first_product, 0)
    pack_start(2)
    for c in near[1:]:
        c.wait()
    for c in b_copies(0):
        c.start()
    for c in far:
        c.start()
    for c in mine:
        c.wait()

    half = rows // 2

    def out_right(s):
        return remote(attb.at[lax.rem(s, 2)], att.at[s, chip], r_send.at[lax.rem(s, 2)], rl_recv.at[s], right)

    def out_left(s):
        return remote(attb.at[lax.rem(s, 2)], att.at[s, chip], l_send.at[lax.rem(s, 2)], rr_recv.at[s], left)

    def out_own(s):
        return local(attb.at[lax.rem(s, 2)], att.at[s, chip], own_sem.at[lax.rem(s, 2)])

    def in_left(s):
        return remote(attb.at[0], att.at[s, before], r_send.at[0], rl_recv.at[s], right)

    def in_right(s):
        return remote(attb.at[0], att.at[s, after], l_send.at[0], rr_recv.at[s], left)

    def pass_right(s):
        part = att.at[s, before, pl.ds(0, half)]
        return remote(part, part, fr_send.at[s], fl_recv.at[s], right)

    def pass_left(s):
        part = att.at[s, after, pl.ds(half, half)]
        return remote(part, part, fl_send.at[s], fr_recv.at[s], left)

    def forward(s):
        in_left(s).wait_recv()
        pass_right(s).start()
        in_right(s).wait_recv()
        pass_left(s).start()

    def body(s, carry):
        g, slot = nseq + s, lax.rem(s, 2)

        @pl.when(s + 1 < nseq)
        def _():
            x_copy(g + 1).start()
            for c in b_copies(s + 1):
                c.start()

        x_copy(g).wait()
        rms_rows(xbuf.at[lax.rem(g, 2)], hbuf, gain, rows, 32)
        for c in mid_copies(s, (before, after, opposite)):
            c.wait_recv()
        mid = dot(sel[...], mids[s]).T.astype(BF16)
        for c in b_copies(s):
            c.wait()
        for p in range(3):
            z = dot_nt(hbuf[...], wbuf[pl.ds(p * width, width), :])
            z = z + scale * dot(mid, bbuf[slot, p])
            qkv[:, pl.ds(p * width, width)] = z.astype(BF16)

        @pl.when((s >= 2) & (s - 2 < keep))
        def _():
            out_right(s - 2).wait_send()
            out_left(s - 2).wait_send()

        @pl.when(s >= 2)
        def _():
            out_own(s - 2).wait()

        attend(qkv, attb.at[slot], width, group, dim, rows // 2)
        out_own(s).start()

        @pl.when(s < keep)
        def _():
            out_right(s).start()
            out_left(s).start()

        for k in range(len(packs)):
            @pl.when(s == k)
            def _(k=k):
                pack_pass(k)

        @pl.when((s >= lag) & (s - lag < keep))
        def _():
            forward(s - lag)

        return carry

    lax.fori_loop(0, nseq, body, 0)
    for k in range(len(packs)):
        pack_across(k)

    def tail(s, carry):
        forward(s)
        return carry

    lax.fori_loop(min(nseq - lag, keep), keep, tail, 0)
    for s in (nseq - 2, nseq - 1):
        if s < keep:
            out_right(s).wait_send()
            out_left(s).wait_send()
        out_own(s).wait()

    def finish(s, carry):
        pass_right(s).wait_send()
        pass_left(s).wait_send()
        got_a, got_b = att.at[s, opposite, pl.ds(0, half)], att.at[s, opposite, pl.ds(half, half)]
        remote(got_a, got_a, fr_send.at[s], fl_recv.at[s], right).wait_recv()
        remote(got_b, got_b, fl_send.at[s], fr_recv.at[s], left).wait_recv()
        return carry

    lax.fori_loop(0, keep, finish, 0)

    def finish_mids(s, carry):
        for c in mid_copies(s):
            c.wait_send()
        return carry

    lax.fori_loop(0, nseq, finish_mids, 0)
    for k in range(len(packs)):
        pack_end(k)
    for c in far:
        c.wait()


def call_a(n, keep, scale, group, dim, share, x, gain, wq, wk, wv, ar, bqkv, wide, agu, wo, wg, wu, wd, lml):
    nseq, rows, model = x.shape[0] // CORES, x.shape[1], x.shape[2]
    own = wq.shape[0]
    width = own * CORES
    rank3, arows = bqkv.shape[1], ar.shape[1]
    crows = CORES * arows
    hbm = pl.BlockSpec(memory_space=pl.ANY)
    vmem = pl.BlockSpec(memory_space=pltpu.VMEM)
    dma = pltpu.SemaphoreType.DMA
    lag = min(3, nseq)
    flops = 2 * nseq * rows * model * (3 * width + rank3)
    return pl.pallas_call(
        functools.partial(kernel_a, n, lag, keep, scale, group, dim, share),
        out_shape=[
            jax.ShapeDtypeStruct((nseq, n, rows, width), BF16),
            jax.ShapeDtypeStruct((nseq, *ar.shape[1:]), BF16),
            jax.ShapeDtypeStruct((nseq, *bqkv.shape[1:]), BF16),
            jax.ShapeDtypeStruct((n, CORES, *wide.shape), BF16),
            jax.ShapeDtypeStruct((n, CORES, *agu.shape), BF16),
            jax.ShapeDtypeStruct((n, CORES, *wo.shape), BF16),
            jax.ShapeDtypeStruct(wg.shape, BF16),
            jax.ShapeDtypeStruct(wu.shape, BF16),
            jax.ShapeDtypeStruct(wd.shape, BF16),
            jax.ShapeDtypeStruct((nseq, *lml.shape[1:]), BF16),
        ],
        in_specs=[hbm, vmem] + [hbm] * 12,
        out_specs=[hbm] * 10,
        scratch_shapes=[
            pltpu.VMEM((3 * width, model), BF16),
            pltpu.VMEM((2, rows, model), BF16),
            pltpu.VMEM((rows, model), BF16),
            pltpu.VMEM((2, crows, model), BF16),
            pltpu.VMEM((2, 3, rank3, width), BF16),
            pltpu.VMEM((rows, 3 * width), BF16),
            pltpu.VMEM((2, rows, width), BF16),
            pltpu.VMEM((nseq, n * crows, rows), BF16),
            pltpu.VMEM((rank3, n * crows), BF16),
            dma((3,)), dma((2,)), dma((2, 2)), dma((2, 3)), dma((2, 3)), dma((5,)), dma((5,)), dma((4,)), dma((4,)),
            dma((3, nseq)), dma((3, nseq)),
        ] + [dma((3,))] * 11 + [
            dma((2,)), dma((2,)), dma((2,)), dma((nseq,)), dma((nseq,)), dma((nseq,)), dma((nseq,)), dma((nseq,)), dma((nseq,)),
        ],
        compiler_params=pltpu.CompilerParams(collective_id=0, has_side_effects=True, vmem_limit_bytes=VMEM_LIMIT),
        cost_estimate=pl.CostEstimate(flops=flops, bytes_accessed=3 * x.size, transcendentals=nseq * rows * rows * width // dim),
        name="qkv_attention",
    )(x, gain, wq, wk, wv, ar, bqkv, wide, agu, wo, wg, wu, wd, lml)


def kernel_b(n, keep, scale, rank, share,
             x, gain, att, wo, wide, agu, wg, wg_o, wu, wu_o, wd, wd_o, lml, lml_o,
             y, att_t,
             wob, gub, wdb, attv, xb, hb, mb, zb, x1b, yb, in1l, in1r, in2l, in2r, aob, bob, agub, lgb, lub, adb, bdb, sel,
             wo_sem, gu_sem, wd_sem, att_sem, x_sem, lo_sem, lg_sem, bd_sem,
             s1r, s1l, s2r, s2l, ar, al, yown, fr, fl, r1l, r1r, r2l, r2r, gl, gr, hl, hr, dsend, drecv,
             t_rs, t_ls, t_rl, t_rr, t_frs, t_fls, t_fl, t_fr):
    core, chip, right, left, partner = ring(n)
    nseq, rows, model = att.shape[0], x.shape[1], x.shape[2]
    width = att.shape[3]
    ff = wg.shape[1]
    first = core * nseq
    ndev, piece_w = wide.shape[0], wide.shape[3]
    late = nseq - keep
    blk = rows // n
    half = blk // 2
    before, after, opposite = lax.rem(chip + n - 1, n), lax.rem(chip + 1, n), lax.rem(chip + 2, n)
    wo_t, gu_t, wd_t = wob.shape[2], gub.shape[3], wdb.shape[2]
    wo_n, gu_n, wd_n = model // wo_t, ff // gu_t, model // wd_t
    greet(right, left, partner)

    def wo_copy(k):
        at = pl.ds(pl.multiple_of(k * wo_t, wo_t), wo_t)
        return local(wo.at[:, at], wob.at[lax.rem(k, 2)], wo_sem.at[lax.rem(k, 2)])

    def gu_copies(k, own):
        at = pl.ds(pl.multiple_of(lax.rem(k, gu_n) * gu_t, gu_t), gu_t)
        slot = lax.rem(k, 2)
        pair = (wg, wu) if own else (wg_o, wu_o)
        return [local(w.at[:, at], gub.at[slot, j], gu_sem.at[slot, j]) for j, w in enumerate(pair)]

    def gu_start(k):
        @pl.when(k < gu_n)
        def _():
            for c in gu_copies(k, True):
                c.start()

        @pl.when(k >= gu_n)
        def _():
            for c in gu_copies(k, False):
                c.start()

    def wd_copies(k):
        at = pl.ds(pl.multiple_of(k * wd_t, wd_t), wd_t)
        slot = lax.rem(k, 2)
        return [local(w.at[:, at], wdb.at[slot, pl.ds(j * ff, ff)], wd_sem.at[slot, j]) for j, w in enumerate((wd, wd_o))]

    def att_copies(s):
        return [local(att.at[s, j], attv.at[:, pl.ds(j * width, width)], att_sem.at[j]) for j in range(n)]

    def att_start(s):
        @pl.when(s < keep)
        def _():
            start(att_copies(s))

        @pl.when(s >= keep)
        def _():
            k = jnp.maximum(s - keep, 0)
            late_in(k)
            for j, own in enumerate(att_copies(s)):
                @pl.when(chip == j)
                def _(own=own):
                    own.start()

                @pl.when(chip != j)
                def _(j=j):
                    local(att_t.at[k, j], attv.at[:, pl.ds(j * width, width)], att_sem.at[j]).start()

    def late_right(k):
        return remote(att.at[keep + k, chip], att_t.at[k, chip], t_rs.at[k], t_rl.at[k], right)

    def late_left(k):
        return remote(att.at[keep + k, chip], att_t.at[k, chip], t_ls.at[k], t_rr.at[k], left)

    def late_hops(k):
        a, b = att_t.at[k, before, pl.ds(0, rows // 2)], att_t.at[k, after, pl.ds(rows // 2, rows // 2)]
        return remote(a, a, t_frs.at[k], t_fl.at[k], right), remote(b, b, t_fls.at[k], t_fr.at[k], left)

    def late_pass(k):
        hop_r, hop_l = late_hops(k)
        remote(att.at[keep + k, chip], att_t.at[k, before], t_rs.at[k], t_rl.at[k], right).wait_recv()
        hop_r.start()
        remote(att.at[keep + k, chip], att_t.at[k, after], t_ls.at[k], t_rr.at[k], left).wait_recv()
        hop_l.start()

    def late_in(k):
        a, b = att_t.at[k, opposite, pl.ds(0, rows // 2)], att_t.at[k, opposite, pl.ds(rows // 2, rows // 2)]
        remote(a, a, t_frs.at[k], t_fl.at[k], right).wait_recv()
        remote(b, b, t_fls.at[k], t_fr.at[k], left).wait_recv()

    def x_copy(s):
        return local(x.at[first + s], xb, x_sem)

    def lora_o(s):
        slot, out = lax.rem(s, 2), []
        for d in range(ndev):
            cols = pl.ds(d * piece_w, piece_w)
            out.append(local(wide.at[d, first + s, pl.ds(0, rank)], aob.at[slot, :, cols], lo_sem.at[slot, 0, d]))
            out.append(local(wide.at[d, first + s, pl.ds(rank, rank)], bob.at[slot, :, cols], lo_sem.at[slot, 1, d]))
            out.append(local(agu.at[d, first + s], agub.at[slot, pl.ds(d * 2 * share, 2 * share)], lo_sem.at[slot, 2, d]))
        return out

    def lora_m(s):
        slot, out = lax.rem(s, 2), []
        for j, (src, k) in enumerate(((lml, first + s), (lml_o, s))):
            at = pl.ds(j * ff, ff)
            out.append(local(src.at[k, pl.ds(0, rank)], lgb.at[slot, pl.ds(0, rank), at], lg_sem.at[slot, 3 * j]))
            out.append(local(src.at[k, pl.ds(rank, rank)], lub.at[slot, pl.ds(rank, rank), at], lg_sem.at[slot, 3 * j + 1]))
            out.append(local(src.at[k, pl.ds(2 * rank, rank)], adb.at[slot, pl.ds(0, rank), at], lg_sem.at[slot, 3 * j + 2]))
        return out

    def start(copies):
        for c in copies:
            c.start()

    def wait(copies):
        for c in copies:
            c.wait()

    def rows_of(j, size=blk, shift=0):
        return pl.ds(pl.multiple_of(j * blk + shift, size), size)

    def rs1_right(s):
        return remote(zb.at[lax.rem(s, 3), rows_of(opposite, half)], in1l.at[lax.rem(s, 3)], s1r.at[s], r1l.at[s], right)

    def rs1_left(s):
        return remote(zb.at[lax.rem(s, 3), rows_of(opposite, half, half)], in1r.at[lax.rem(s, 3)], s1l.at[s], r1r.at[s], left)

    def rs2_right(s):
        return remote(zb.at[lax.rem(s, 3), rows_of(after)], in2l.at[lax.rem(s, 3)], s2r.at[s], r2l.at[s], right)

    def rs2_left(s):
        return remote(zb.at[lax.rem(s, 3), rows_of(before)], in2r.at[lax.rem(s, 3)], s2l.at[s], r2r.at[s], left)

    def ag1_right(s):
        return remote(yb.at[lax.rem(s, 2)], y.at[first + s, rows_of(chip)], ar.at[s], gl.at[s], right)

    def ag1_left(s):
        return remote(yb.at[lax.rem(s, 2)], y.at[first + s, rows_of(chip)], al.at[s], gr.at[s], left)

    def ag1_own(s):
        return local(yb.at[lax.rem(s, 2)], y.at[first + s, rows_of(chip)], yown.at[s])

    def ag2_right(s, block):
        part = y.at[first + s, rows_of(block, half)]
        return remote(part, part, fr.at[s], hl.at[s], right)

    def ag2_left(s, block):
        part = y.at[first + s, rows_of(block, half, half)]
        return remote(part, part, fl.at[s], hr.at[s], left)

    def across(s, k, block):
        part = y.at[first + s, rows_of(block)]
        return remote(yb.at[lax.rem(s, 2)] if k == 0 else part, part, dsend.at[k, s], drecv.at[k, s], partner)

    def across_in(s, k):
        there = y.at[(1 - core) * nseq + s, rows_of((chip, before, after, opposite)[k])]
        return remote(there, there, dsend.at[k, s], drecv.at[k, s], partner)

    def do_rs2(s):
        slot = lax.rem(s, 3)
        rs1_right(s).wait_recv()
        at = rows_of(after, half)
        zb[slot, at, :] = (zb[slot, at, :].astype(F32) + in1l[slot].astype(F32)).astype(BF16)
        rs2_right(s).start()
        rs1_left(s).wait_recv()
        at = rows_of(before, half, half)
        zb[slot, at, :] = (zb[slot, at, :].astype(F32) + in1r[slot].astype(F32)).astype(BF16)
        rs2_left(s).start()

    def do_rs3(s):
        slot, yslot = lax.rem(s, 3), lax.rem(s, 2)

        @pl.when(s >= 2)
        def _():
            ag1_right(s - 2).wait_send()
            ag1_left(s - 2).wait_send()
            ag1_own(s - 2).wait()
            across(s - 2, 0, chip).wait_send()

        rs2_right(s).wait_recv()
        rs2_left(s).wait_recv()
        mine = zb.at[slot, rows_of(chip)]
        tail = pl.ds(model, 128)
        mid = mine[:, tail].astype(F32) + in2l[slot, :, tail].astype(F32) + in2r[slot, :, tail].astype(F32)
        mid = mid.astype(BF16)[:, :rank]

        def piece(k, carry):
            at = pl.ds(pl.multiple_of(k * wo_t, wo_t), wo_t)
            z = mine[:, at].astype(F32) + in2l[slot, :, at].astype(F32) + in2r[slot, :, at].astype(F32)
            z = z + scale * dot(mid, bdb[s, :, at])
            yb[yslot, :, at] = (x1b[slot, :, at].astype(F32) + z).astype(BF16)
            return carry

        lax.fori_loop(0, wo_n, piece, 0)
        ag1_right(s).start()
        ag1_left(s).start()
        ag1_own(s).start()
        across(s, 0, chip).start()

    def do_ag2(s):
        remote(yb.at[0], y.at[first + s, rows_of(before)], ar.at[s], gl.at[s], right).wait_recv()
        ag2_right(s, before).start()
        across(s, 1, before).start()
        remote(yb.at[0], y.at[first + s, rows_of(after)], al.at[s], gr.at[s], left).wait_recv()
        ag2_left(s, after).start()
        across(s, 2, after).start()

    def do_across(s):
        ag2_right(s, opposite).wait_recv()
        ag2_left(s, opposite).wait_recv()
        across(s, 3, opposite).start()

    def when(cond, f, s):
        @pl.when(cond)
        def _():
            f(s)

    for k in range(late):
        late_right(k).start()
        late_left(k).start()
    bd_copies = [local(wide.at[d, pl.ds(first, nseq), pl.ds(2 * rank, rank)], bdb.at[:, :, pl.ds(d * piece_w, piece_w)],
                       bd_sem.at[d]) for d in range(ndev)]
    start(bd_copies)
    sel[...] = pick(sel.shape, share, rank, 2, 0)
    for k in range(2):
        wo_copy(k).start()
        start(gu_copies(k, True))
        start(wd_copies(k))
    start(att_copies(0))
    x_copy(0).start()
    start(lora_o(0))
    lgb[...] = jnp.zeros_like(lgb)
    lub[...] = jnp.zeros_like(lub)
    adb[...] = jnp.zeros_like(adb)
    start(lora_m(0))
    wait(bd_copies)

    def out_proj(s):
        slot = lax.rem(s, 2)
        wait(lora_o(s))
        wait(att_copies(s))
        x_copy(s).wait()
        mid = dot_nt(attv[...], aob[slot]).astype(BF16)

        def tile(k, carry):
            at = pl.ds(pl.multiple_of(k * wo_t, wo_t), wo_t)
            wo_copy(k).wait()
            z = dot(attv[...], wob[lax.rem(k, 2)]) + scale * dot(mid, bob[slot, :, at])
            xb[:, at] = (xb[:, at].astype(F32) + z).astype(BF16)

            @pl.when((k + 2 < wo_n) | (s + 1 < nseq))
            def _():
                wo_copy(lax.rem(k + 2, wo_n)).start()

            return carry

        lax.fori_loop(0, wo_n, tile, 0)
        rms_rows(xb, hb, gain, rows, 32)
        x1b[lax.rem(s, 3)] = xb[rows_of(chip), :]

        @pl.when(s + 1 < nseq)
        def _():
            att_start(s + 1)
            x_copy(s + 1).start()

    def gate_up(s):
        slot = lax.rem(s, 2)
        mid = dot_nt(hb[...], agub[slot]).astype(BF16)
        mid = dot(mid, sel[...]).astype(BF16)

        @pl.when(s + 1 < nseq)
        def _():
            start(lora_o(s + 1))

        wait(lora_m(s))

        def tile(k, carry):
            at = pl.ds(pl.multiple_of(k * gu_t, gu_t), gu_t)
            wait(gu_copies(k, True))
            g = dot(hb[...], gub[lax.rem(k, 2), 0]) + scale * dot(mid, lgb[slot, :, at])
            u = dot(hb[...], gub[lax.rem(k, 2), 1]) + scale * dot(mid, lub[slot, :, at])
            g = g.astype(BF16).astype(F32)
            u = u.astype(BF16).astype(F32)
            mb[:, at] = (jax.nn.silu(g) * u).astype(BF16)

            @pl.when((k + 2 < 2 * gu_n) | (s + 1 < nseq))
            def _():
                gu_start(lax.rem(k + 2, 2 * gu_n))

            return carry

        lax.fori_loop(0, 2 * gu_n, tile, 0)

        @pl.when(s + 1 < nseq)
        def _():
            start(lora_m(s + 1))

    def down(s):
        slot = lax.rem(s, 3)

        @pl.when(s >= 3)
        def _():
            rs1_right(s - 3).wait_send()
            rs1_left(s - 3).wait_send()
            rs2_right(s - 3).wait_send()
            rs2_left(s - 3).wait_send()

        zb[slot, :, pl.ds(model, 128)] = dot_nt(mb[...], adb[lax.rem(s, 2)]).astype(BF16)

        def tile(k, carry):
            at = pl.ds(pl.multiple_of(k * wd_t, wd_t), wd_t)
            wait(wd_copies(k))
            zb[slot, :, at] = dot(mb[...], wdb[lax.rem(k, 2)]).astype(BF16)

            @pl.when((k + 2 < wd_n) | (s + 1 < nseq))
            def _():
                start(wd_copies(lax.rem(k + 2, wd_n)))

            return carry

        lax.fori_loop(0, wd_n, tile, 0)
        rs1_right(s).start()
        rs1_left(s).start()

    def body(t, carry):
        when((t >= 4) & (t < nseq + 4), do_across, t - 4)
        when((t >= 3) & (t < nseq + 3), do_ag2, t - 3)
        when(t < nseq, out_proj, t)
        when((t >= 1) & (t < nseq + 1), do_rs2, t - 1)
        when(t < nseq, gate_up, t)
        if late > 0:
            when(t == 0, lambda _: late_pass(0), t)
        when((t >= 2) & (t < nseq + 2), do_rs3, t - 2)
        when(t < nseq, down, t)
        for k in range(1, late):
            when(t == k - 1, lambda _, k=k: late_pass(k), t)
        return carry

    lax.fori_loop(0, nseq + 4, body, 0)

    for s in range(max(nseq - 3, 0), nseq):
        rs1_right(s).wait_send()
        rs1_left(s).wait_send()
        rs2_right(s).wait_send()
        rs2_left(s).wait_send()
    for s in range(max(nseq - 2, 0), nseq):
        ag1_right(s).wait_send()
        ag1_left(s).wait_send()
        ag1_own(s).wait()
        across(s, 0, chip).wait_send()

    def finish(s, carry):
        ag2_right(s, before).wait_send()
        ag2_left(s, after).wait_send()
        for k, block in ((1, before), (2, after), (3, opposite)):
            across(s, k, block).wait_send()
        for k in range(4):
            across_in(s, k).wait_recv()
        return carry

    lax.fori_loop(0, nseq, finish, 0)
    for k in range(late):
        late_right(k).wait_send()
        late_left(k).wait_send()
        for hop in late_hops(k):
            hop.wait_send()


def call_b(n, keep, scale, rank, share, x, gain, att, wo, wide, agu, wg, wg_o, wu, wu_o, wd, wd_o, lml, lml_o):
    nseq, rows, model, ff = att.shape[0], x.shape[1], x.shape[2], wg.shape[1]
    hbm = pl.BlockSpec(memory_space=pl.ANY)
    vmem = pl.BlockSpec(memory_space=pltpu.VMEM)
    dma = pltpu.SemaphoreType.DMA
    blk = rows // n
    ndev = wide.shape[0]
    zwide = model + 128
    tile = 512
    flops = 2 * nseq * rows * (model * model + 3 * model * ff * CORES)
    return pl.pallas_call(
        functools.partial(kernel_b, n, keep, scale, rank, share),
        out_shape=[jax.ShapeDtypeStruct(x.shape, BF16), jax.ShapeDtypeStruct((nseq - keep, *att.shape[1:]), BF16)],
        in_specs=[hbm, vmem] + [hbm] * 12,
        out_specs=[hbm] * 2,
        scratch_shapes=[
            pltpu.VMEM((2, model, tile), BF16),
            pltpu.VMEM((2, 2, model, tile // 2), BF16),
            pltpu.VMEM((2, CORES * ff, tile), BF16),
            pltpu.VMEM((rows, model), BF16),
            pltpu.VMEM((rows, model), BF16),
            pltpu.VMEM((rows, model), BF16),
            pltpu.VMEM((rows, CORES * ff), BF16),
            pltpu.VMEM((3, rows, zwide), BF16),
            pltpu.VMEM((3, blk, model), BF16),
            pltpu.VMEM((2, blk, model), BF16),
            pltpu.VMEM((3, blk // 2, zwide), BF16),
            pltpu.VMEM((3, blk // 2, zwide), BF16),
            pltpu.VMEM((3, blk, zwide), BF16),
            pltpu.VMEM((3, blk, zwide), BF16),
            pltpu.VMEM((2, rank, model), BF16),
            pltpu.VMEM((2, rank, model), BF16),
            pltpu.VMEM((2, 2 * rank, model), BF16),
            pltpu.VMEM((2, 2 * rank, CORES * ff), BF16),
            pltpu.VMEM((2, 2 * rank, CORES * ff), BF16),
            pltpu.VMEM((2, 128, CORES * ff), BF16),
            pltpu.VMEM((nseq, rank, model), BF16),
            pltpu.VMEM((2 * rank, 2 * rank), BF16),
            dma((2,)), dma((2, 2)), dma((2, 2)), dma((n,)), dma, dma((2, 3, ndev)), dma((2, 6)), dma((ndev,)),
        ] + [dma((nseq,))] * 17 + [dma((4, nseq))] * 2 + [dma((nseq - keep,))] * 8,
        compiler_params=pltpu.CompilerParams(collective_id=1, has_side_effects=True, vmem_limit_bytes=VMEM_LIMIT),
        cost_estimate=pl.CostEstimate(flops=flops, bytes_accessed=4 * x.size, transcendentals=0),
        name="out_mlp",
    )(x, gain, att, wo, wide, agu, wg, wg_o, wu, wu_o, wd, wd_o, lml, lml_o)[0]


def solution(mesh):
    n = mesh.shape["tp"] // CORES
    act_spec = P("dp", None, None)
    w_head, w_out, w_col, w_row = P(None, "tp", None), P("tp", None, None), P(None, "tp"), P("tp", None)
    a_rank, b_head, b_col = P(None, None, "tp"), P(None, None, "tp", None), P(None, None, "tp")
    a_head, a_row = P(None, "tp", None, None), P(None, "tp", None)
    in_specs = (act_spec, P("dp"), P(None), P(None), w_head, w_head, w_head, w_out, w_col, w_col, w_row,
                a_rank, b_head, a_rank, b_head, a_rank, b_head, a_head, b_col, a_rank, b_col, a_rank, b_col, a_row, b_col)

    def local_layer(x_in, adapter_ids, gain_attn, gain_mlp, w_q, w_k, w_v, w_o, w_gate, w_up, w_down,
                    a_q, b_q, a_k, b_k, a_v, b_v, a_o, b_o, a_gate, b_gate, a_up, b_up, a_down, b_down):
        nseq, model = x_in.shape[0], x_in.shape[2]
        rank, dim = b_q.shape[1], w_q.shape[2]
        own = w_q.shape[1] * dim
        scale = LORA_ALPHA / rank
        share = a_q.shape[2]
        group = math.lcm(dim, 128) // dim
        keep = max(nseq // CORES - 2, 1)

        def take(*stacks):
            return jnp.take(jnp.concatenate(stacks, axis=1), adapter_ids, axis=0, mode="clip")

        def turn(stack):
            return jnp.swapaxes(stack, 1, 2)

        ar = take(turn(a_q), turn(a_k), turn(a_v), jnp.zeros((a_q.shape[0], share, model), BF16))
        bqkv = take(*[b.reshape(-1, rank, own) for b in (b_q, b_k, b_v)])
        wide = take(turn(a_o.reshape(-1, own, rank)), b_o, b_down)
        agu = take(turn(a_gate), turn(a_up))
        lml = take(b_gate, b_up, turn(a_down))
        flat = [jnp.transpose(w, (1, 2, 0)).reshape(own, model) for w in (w_q, w_k, w_v)]
        att, _, _, wide_f, agu_f, wo_f, wg_o, wu_o, wd_o, lml_o = call_a(
            n, keep, scale, group, dim, share, x_in, gain_attn.reshape(1, model), *flat, ar, bqkv, wide, agu,
            w_o.reshape(own, model), w_gate, w_up, w_down, lml)
        return call_b(n, keep, scale, rank, share, x_in, gain_mlp.reshape(1, model), att, wo_f.reshape(-1, model),
                      wide_f.reshape(-1, *wide.shape), agu_f.reshape(-1, *agu.shape), w_gate, wg_o, w_up, wu_o, w_down, wd_o,
                      lml, lml_o)

    return jax.shard_map(local_layer, mesh=mesh, in_specs=in_specs, out_specs=act_spec, check_vma=False)
```

```python
import functools
import math

import jax
import jax.numpy as jnp
from jax import lax
from jax.experimental import pallas as pl
from jax.experimental.pallas import tpu as pltpu
from jax.sharding import PartitionSpec as P

LORA_ALPHA = 16
RMS_EPS = 1e-5
CORES = 2
MESH = pl.DeviceIdType.MESH
F32, BF16 = jnp.float32, jnp.bfloat16
NT = (((1,), (1,)), ((), ()))
VMEM_LIMIT = 67_000_000
PAIR, TRIPLE, QUAD = 2, 3, 4
LANES = 128
N = None


def even(k):
    return lax.rem(k, PAIR)


def third(k):
    return lax.rem(k, TRIPLE)


def head(size):
    return pl.ds(0, size)


def loop(count, body, start):
    return lax.fori_loop(0, count, body, start)


def dot(a, b):
    return jnp.dot(a, b, preferred_element_type=F32)


def dot_nt(a, b):
    return lax.dot_general(a, b, NT, preferred_element_type=F32)


def ring(n):
    me = lax.axis_index("tp")
    core, chip = lax.rem(me, CORES), lax.div(me, CORES)
    right = lax.rem(chip + 1, n) * CORES + core
    left = lax.rem(chip + n - 1, n) * CORES + core
    return core, chip, right, left, chip * CORES + 1 - core


def greet(*others):
    barrier = pltpu.get_barrier_semaphore()
    for other in others:
        pl.semaphore_signal(barrier, inc=1, device_id={"tp": other}, device_id_type=MESH)
    pl.semaphore_wait(barrier, len(others))


def remote(src, dst, send, recv, to):
    return pltpu.make_async_remote_copy(src_ref=src, dst_ref=dst, send_sem=send, recv_sem=recv, device_id={"tp": to},
                                        device_id_type=MESH)


def local(src, dst, sem):
    return pltpu.make_async_copy(src, dst, sem)


def rms_rows(src, dst, gain, rows, step):
    def chunk(k, carry):
        at = pl.ds(pl.multiple_of(k * step, step), step)
        v = src[at, :].astype(F32)
        inv = lax.rsqrt(jnp.mean(v * v, axis=-1, keepdims=True) + RMS_EPS)
        dst[at, :] = (v * inv * gain[...]).astype(BF16)
        return carry

    loop(rows // step, chunk, 0)


def head_windows(group, dim):
    out = []
    for h in range(group):
        lo, hi = h * dim, (h + 1) * dim
        start, stop = lo // 128 * 128, -(-hi // 128) * 128
        out.append((start, stop, lo - start, hi - start))
    return out


def attend(qkv, out, width, group, dim, qblock):
    seq = qkv.shape[0]
    lanes = group * dim

    def one_group(g, carry):
        base = pl.multiple_of(g * lanes, 128)
        for qb in range(seq // qblock):
            rows, keys = pl.ds(qb * qblock, qblock), (qb + 1) * qblock
            acc = [None] * (lanes // 128)
            mask = (lax.broadcasted_iota(jnp.int32, (qblock, keys), 0) + qb * qblock
                    >= lax.broadcasted_iota(jnp.int32, (qblock, keys), 1))
            for start, stop, lo, hi in head_windows(group, dim):
                size = stop - start
                lane_q = lax.broadcasted_iota(jnp.int32, (qblock, size), 1)
                lane_k = lax.broadcasted_iota(jnp.int32, (keys, size), 1)
                q = qkv[rows, pl.ds(base + start, size)]
                k = qkv[head(keys), pl.ds(width + base + start, size)]
                v = qkv[head(keys), pl.ds(2 * width + base + start, size)]
                q = jnp.where((lane_q >= lo) & (lane_q < hi), q, jnp.zeros_like(q))
                v = jnp.where((lane_k >= lo) & (lane_k < hi), v, jnp.zeros_like(v))
                scores = jnp.where(mask, dot_nt(q, k) * dim ** -0.5, -jnp.inf)
                top = jnp.max(scores, axis=-1, keepdims=True)
                e = jnp.exp(scores - top)
                prob = (e / jnp.sum(e, axis=-1, keepdims=True)).astype(BF16)
                o = dot(prob, v)
                for t in range(size // 128):
                    piece = o[:, t * 128:(t + 1) * 128]
                    j = start // 128 + t
                    acc[j] = piece if acc[j] is None else acc[j] + piece
            for j, piece in enumerate(acc):
                out[rows, pl.ds(base + j * 128, 128)] = piece.astype(BF16)
        return carry

    loop(width // lanes, one_group, 0)


def pick(shape, share, ranks, slots, axis):
    i = lax.broadcasted_iota(jnp.int32, shape, axis)
    t = lax.broadcasted_iota(jnp.int32, shape, 1 - axis)
    dev, slot, r = i // (slots * share), (i // share) % slots, i % share
    return jnp.where(t == slot * ranks + dev * share + r, 1.0, 0.0).astype(BF16)


class OutStage:
    def __init__(self, n, scale, rank, share, x, gain, wo_refs, wide_refs, agu_refs, bufs, wo_sem, lo_sem):
        self.core, self.chip, *_ = ring(n)
        self.before, self.after = lax.rem(self.chip + n - 1, n), lax.rem(self.chip + 1, n)
        self.opposite = lax.rem(self.chip + 2, n)
        self.scale, self.rank, self.share, self.x, self.gain = scale, rank, share, x, gain
        self.wide_refs, self.agu_refs, self.bufs = wide_refs, agu_refs, bufs
        self.wo_sem, self.lo_sem = wo_sem, lo_sem
        self.rows, self.first = x.shape[1], self.core * (x.shape[0] // CORES)
        wo, wo_l, wo_r, wo_f, wo_x = wo_refs
        hi, deep = wo_l.shape[0], wo.shape[0]
        self.width = wide_refs[0].shape[2]
        self.tile_w = bufs[0].shape[2]
        self.tiles_n = x.shape[2] // self.tile_w
        chips = (self.chip, self.before, self.after, self.opposite)
        self.shares = [(CORES * c + self.core, 0, j) for j, c in enumerate(chips)]
        self.shares += [(CORES * c + 1 - self.core, 1, j) for j, c in enumerate(chips)]
        self.wo_shares = []
        for d, cross, j in self.shares:
            base = pl.multiple_of(d * deep, deep)
            if cross or j in (0, 3):
                self.wo_shares.append((self.share_of((wo, wo_f, wo_x), cross, j), pl.ds(base, deep)))
            else:
                self.wo_shares.append(((wo_l, wo_r)[j - 1], pl.ds(base, hi)))
                self.wo_shares.append((wo_f.at[j - 1, pl.ds(hi, deep - hi)], pl.ds(base + hi, deep - hi)))

    @staticmethod
    def share_of(refs, cross, j):
        return refs[2].at[j] if cross else refs[0] if j == 0 else refs[1].at[j - 1]

    def cols(self, d):
        return pl.ds(pl.multiple_of(d * self.width, self.width), self.width)

    def wo_copies(self, k):
        wob = self.bufs[0]
        at, slot = pl.ds(pl.multiple_of(k * self.tile_w, self.tile_w), self.tile_w), even(k)
        return [local(src.at[:, at], wob.at[slot, rows_at], self.wo_sem.at[slot, j])
                for j, (src, rows_at) in enumerate(self.wo_shares)]

    def lora(self, s, slot):
        _, _, _, _, aob, bob, agub = self.bufs
        rank, out = self.rank, []
        for d, cross, j in self.shares:
            src = self.share_of(self.wide_refs, cross, j).at[s if cross else self.first + s]
            out.append(local(src.at[head(rank)], aob.at[slot, :, self.cols(d)], self.lo_sem.at[slot, 0, 4 * cross + j]))
            out.append(local(src.at[pl.ds(rank, rank)], bob.at[slot, :, self.cols(d)], self.lo_sem.at[slot, 1, 4 * cross + j]))
        for i, (j, src, k) in enumerate(((self.core, self.agu_refs[0], self.first + s), (1 - self.core, self.agu_refs[1], s))):
            rows_at = pl.ds(pl.multiple_of(j * 2 * self.share, 2 * self.share), 2 * self.share)
            out.append(local(src.at[k], agub.at[slot, rows_at], self.lo_sem.at[slot, 2, i]))
        return out

    def first_product(self, slot):
        _, attv, _, mido, aob, _, _ = self.bufs
        mido[...] = dot_nt(attv[...], aob[slot]).astype(BF16)

    def tiles(self, slot, lo, hi, more):
        wob, attv, xb, mido, _, bob, _ = self.bufs
        mid = mido[...]

        def tile(k, carry):
            at = pl.ds(pl.multiple_of(k * self.tile_w, self.tile_w), self.tile_w)
            for c in self.wo_copies(k):
                c.wait()
            z = dot(attv[...], wob[even(k)]) + self.scale * dot(mid, bob[slot, :, at])
            xb[:, at] = (xb[:, at].astype(F32) + z).astype(BF16)

            @pl.when((k + 2 < self.tiles_n) | more)
            def _():
                for c in self.wo_copies(lax.rem(k + 2, self.tiles_n)):
                    c.start()

            return carry

        lax.fori_loop(lo, hi, tile, 0)

    def norm(self, slot, h, mid_rows):
        _, _, xb, _, _, _, agub = self.bufs
        rms_rows(xb, h, self.gain, self.rows, 64)
        mid_rows[...] = dot_nt(agub[slot], h[...]).astype(BF16)


def kernel_a(n, lag, keep, scale, group, dim, share,
             x, gain, gain_mlp, wq, wk, wv, ar, agu, bqkv, wide, wo, wo_l, wo_r, wg, wu, wd, lml,
             att, ar_oth, agu_oth, b_oth, wide_f, wide_x, wo_f, wo_x, wg_o, wu_o, wd_o, lml_o, h_out, x1_out, mg_out,
             wbuf, xbuf, hbuf, abuf, bbuf, qkv, attb, mids, sel, wob, attv, xb, hb, mido, aob, bob, agub, mgu,
             w_sem, x_sem, a_sem, bo_sem, bp_sem, d_send, d_recv, o_send, o_recv, m_send, m_recv,
             pr_send, pl_send, prl_recv, prr_recv, pfr_send, pfl_send, pfl_recv, pfr_recv, pp_send, pp_recv,
             r_send, l_send, own_sem, rl_recv, rr_recv, fr_send, fl_send, fl_recv, fr_recv,
             wo_sem, lo_sem, att_sem, xo_sem, g_send, g_recv, e_sem):
    core, chip, right, left, partner = ring(n)
    before, after, opposite = lax.rem(chip + n - 1, n), lax.rem(chip + 1, n), lax.rem(chip + 2, n)
    across = opposite * CORES + core
    nseq, rows, own = x.shape[0] // CORES, x.shape[1], wq.shape[0]
    width = own * CORES
    first = core * nseq
    rank = bqkv.shape[1] // 3
    arows = ar.shape[1]
    crows = CORES * arows
    greet(right, left, partner, across)

    theirs, mine_at = pl.ds((1 - core) * nseq, nseq), pl.ds(first, nseq)
    near = [remote(ar.at[theirs], ar_oth, d_send.at[4], d_recv.at[4], partner)]
    near += [remote(w, wbuf.at[pl.ds(p * width + core * own, own)], d_send.at[p], d_recv.at[p], partner)
             for p, w in enumerate((wq, wk, wv))]
    near.append(remote(bqkv.at[theirs], b_oth, d_send.at[3], d_recv.at[3], partner))
    far = [remote(src, dst, o_send.at[k], o_recv.at[k], partner)
           for k, (src, dst) in enumerate(((lml.at[theirs], lml_o), (wg, wg_o), (wu, wu_o), (wd, wd_o),
                                     (agu.at[theirs], agu_oth)))]
    mine = [local(w, wbuf.at[pl.ds(p * width + core * own, own)], w_sem.at[p]) for p, w in enumerate((wq, wk, wv))]

    hi = wo_l.shape[0]
    whole, top, low = head(wo.shape[0]), head(hi), pl.ds(hi, wo.shape[0] - hi)
    wide_half = wide.shape[0] // 2
    to_right, to_left = (right, pr_send, prl_recv, pfr_send, pfl_recv), (left, pl_send, prr_recv, pfl_send, pfr_recv)

    def pack_first(k, way):
        to, send, recv, _, _ = (to_right, to_left)[way]
        if k == 0:
            return remote(wide, wide_f.at[way], send.at[k], recv.at[k], to)
        return remote(wo.at[low], wo_f.at[way, low], send.at[k], recv.at[k], to)

    def pack_second(k, way):
        to, _, _, send, recv = (to_right, to_left)[way]
        if k == 0:
            part = pl.ds(way * wide_half, wide_half)
            return remote(wide_f.at[way, part], wide_f.at[2, part], send.at[k], recv.at[k], to)
        part = (top, low)[way]
        return remote(wo_l if way == 0 else wo_f.at[1, low], wo_f.at[2, part], send.at[k], recv.at[k], to)

    def wide_push(j):
        src = wide if j == 0 else wide_f.at[j - 1]
        return remote(src.at[theirs], wide_x.at[j], pp_send.at[j], pp_recv.at[j], partner)

    def wo_push(j):
        src, dst = ((wo, wo_x.at[0]), (wo_l, wo_x.at[1, top]), (wo_r, wo_x.at[2, top]), (wo_f.at[0, low], wo_x.at[1, low]),
                    (wo_f.at[1, low], wo_x.at[2, low]), (wo_f.at[2], wo_x.at[3]))[j]
        return remote(src, dst, pp_send.at[4 + j], pp_recv.at[4 + j], partner)

    def pack_start(k):
        for way in range(2):
            pack_first(k, way).start()
        if k == 0:
            wide_push(0).start()
        else:
            for j in range(3):
                wo_push(j).start()

    def pack_pass(k):
        for way in range(2):
            pack_first(k, way).wait_recv()
            if k == 0 or way == 1:
                pack_second(k, way).start()
            (wide_push(way + 1) if k == 0 else wo_push(way + 3)).start()

    def pack_across(k):
        for way in range(2):
            pack_second(k, way).wait_recv()
        (wide_push(3) if k == 0 else wo_push(5)).start()

    def wo_ready():
        for j in range(4):
            wide_push(j).wait_recv()
        for j in range(6):
            wo_push(j).wait_recv()
        far[4].wait_recv()

    def pack_end():
        for k in range(2):
            for way in range(2):
                pack_first(k, way).wait_send()
                pack_second(k, way).wait_send()
        for j in range(4):
            wide_push(j).wait_send()
        for j in range(6):
            wo_push(j).wait_send()

    def x_copy(g):
        return local(x.at[first + lax.rem(g, nseq)], xbuf.at[even(g)], x_sem.at[even(g)])

    def a_copies(s):
        slot = even(s)
        own_at = pl.ds(pl.multiple_of(core * arows, arows), arows)
        oth_at = pl.ds(pl.multiple_of((1 - core) * arows, arows), arows)
        return [local(ar.at[first + s], abuf.at[slot, own_at], a_sem.at[slot, 0]),
                local(ar_oth.at[s], abuf.at[slot, oth_at], a_sem.at[slot, 1])]

    def b_copies(s):
        slot, out = even(s), []
        for p in range(3):
            part = pl.ds(p * rank, rank)
            own_at = pl.ds(pl.multiple_of(core * own, 128), own)
            oth_at = pl.ds(pl.multiple_of((1 - core) * own, 128), own)
            out.append(local(bqkv.at[first + s, part], bbuf.at[slot, p, part, own_at], bo_sem.at[slot, p]))
            out.append(local(b_oth.at[s, part], bbuf.at[slot, p, part, oth_at], bp_sem.at[slot, p]))
        return out

    near[0].start()
    pack_start(0)
    for c in near[1:] + mine:
        c.start()
    x_copy(0).start()
    bbuf[...] = jnp.zeros_like(bbuf)
    sel[...] = pick(sel.shape, share, rank, arows // share, 1)
    near[0].wait()
    for c in a_copies(0):
        c.start()

    def rank_rows(j):
        return pl.ds(pl.multiple_of(j * crows, crows), crows)

    def mid_copies(s, source=None):
        froms = (chip, chip, chip) if source is None else source
        return [remote(mids.at[s, rank_rows(j)], mids.at[s, rank_rows(j)], m_send.at[k, s], m_recv.at[k, s], to)
                for k, (j, to) in enumerate(zip(froms, (right, left, across)))]

    def first_product(s, carry):
        slot = even(s)
        x_copy(s + 1).start()

        @pl.when(s + 1 < nseq)
        def _():
            for c in a_copies(s + 1):
                c.start()

        @pl.when(s == nseq // 2)
        def _():
            pack_start(1)

        x_copy(s).wait()
        rms_rows(xbuf.at[slot], hbuf, gain, rows, 32)
        for c in a_copies(s):
            c.wait()
        mids[s, rank_rows(chip), :] = dot_nt(abuf[slot], hbuf[...]).astype(BF16)
        for c in mid_copies(s):
            c.start()
        return carry

    loop(nseq, first_product, 0)
    pack_second(1, 0).start()
    for c in near[1:]:
        c.wait()
    for c in b_copies(0):
        c.start()
    for c in far:
        c.start()
    for c in mine:
        c.wait()

    half = rows // 2

    def out_right(s):
        return remote(attb.at[even(s)], att.at[s, chip], r_send.at[even(s)], rl_recv.at[s], right)

    def out_left(s):
        return remote(attb.at[even(s)], att.at[s, chip], l_send.at[even(s)], rr_recv.at[s], left)

    def out_own(s):
        return local(attb.at[even(s)], att.at[s, chip], own_sem.at[even(s)])

    def in_left(s):
        return remote(attb.at[0], att.at[s, before], r_send.at[0], rl_recv.at[s], right)

    def in_right(s):
        return remote(attb.at[0], att.at[s, after], l_send.at[0], rr_recv.at[s], left)

    def pass_right(s):
        part = att.at[s, before, head(half)]
        return remote(part, part, fr_send.at[s], fl_recv.at[s], right)

    def pass_left(s):
        part = att.at[s, after, pl.ds(half, half)]
        return remote(part, part, fl_send.at[s], fr_recv.at[s], left)

    def forward(s):
        in_left(s).wait_recv()
        pass_right(s).start()
        in_right(s).wait_recv()
        pass_left(s).start()

    def gathered(s):
        got_a, got_b = att.at[s, opposite, head(half)], att.at[s, opposite, pl.ds(half, half)]
        remote(got_a, got_a, fr_send.at[s], fl_recv.at[s], right).wait_recv()
        remote(got_b, got_b, fl_send.at[s], fr_recv.at[s], left).wait_recv()

    grows = CORES * 2 * share
    blk = rows // n

    def group_rows(j):
        return pl.ds(pl.multiple_of(j * grows, grows), grows)

    def gate_mids(froms):
        return [remote(mgu.at[group_rows(j)], mgu.at[group_rows(j)], g_send.at[k], g_recv.at[k], to)
                for k, (j, to) in enumerate(zip(froms, (right, left, across)))]

    def exports():
        return [local(hb, h_out, e_sem.at[0]),
                local(xb.at[pl.ds(pl.multiple_of(chip * blk, blk), blk)], x1_out, e_sem.at[1])]

    def first_out():
        stage = OutStage(n, scale, rank, share, x, gain_mlp, (wo, wo_l, wo_r, wo_f, wo_x), (wide, wide_f, wide_x),
                         (agu, agu_oth), (wob, attv, xb, mido, aob, bob, agub), wo_sem, lo_sem)
        wo_ready()
        gathered(0)
        loads = [local(att.at[0, j], attv.at[:, pl.ds(j * width, width)], att_sem.at[j]) for j in range(n)]
        loads += [local(x.at[first], xb, xo_sem)] + stage.lora(0, 0)
        for c in loads + stage.wo_copies(0) + stage.wo_copies(1):
            c.start()
        for c in loads:
            c.wait()
        stage.first_product(0)
        stage.tiles(0, 0, stage.tiles_n, False)
        stage.norm(0, hb, mgu.at[group_rows(chip)])
        for c in gate_mids((chip, chip, chip)) + exports():
            c.start()

    def body(s, carry):
        g, slot = nseq + s, even(s)

        @pl.when(s + 1 < nseq)
        def _():
            x_copy(g + 1).start()
            for c in b_copies(s + 1):
                c.start()

        x_copy(g).wait()
        rms_rows(xbuf.at[even(g)], hbuf, gain, rows, 32)
        for c in mid_copies(s, (before, after, opposite)):
            c.wait_recv()
        mid = dot(sel[...], mids[s]).T.astype(BF16)
        for c in b_copies(s):
            c.wait()
        for p in range(3):
            z = dot_nt(hbuf[...], wbuf[pl.ds(p * width, width), :])
            z = z + scale * dot(mid, bbuf[slot, p])
            qkv[:, pl.ds(p * width, width)] = z.astype(BF16)

        @pl.when((s >= 2) & (s - 2 < keep))
        def _():
            out_right(s - 2).wait_send()
            out_left(s - 2).wait_send()

        @pl.when(s >= 2)
        def _():
            out_own(s - 2).wait()

        attend(qkv, attb.at[slot], width, group, dim, rows // 2)
        out_own(s).start()

        @pl.when(s < keep)
        def _():
            out_right(s).start()
            out_left(s).start()

        @pl.when(s == 0)
        def _():
            for k in range(2):
                pack_pass(k)


        @pl.when((s >= lag) & (s - lag < keep))
        def _():
            forward(s - lag)

        @pl.when(s == nseq - 2)
        def _():
            for k in range(2):
                pack_across(k)

        return carry

    loop(nseq, body, 0)

    def tail(s, carry):
        forward(s)
        return carry

    lax.fori_loop(max(min(nseq - lag, keep), 0), keep, tail, 0)
    first_out()
    for s in (nseq - 2, nseq - 1):
        if s < keep:
            out_right(s).wait_send()
            out_left(s).wait_send()
        out_own(s).wait()

    def finish(s, carry):
        pass_right(s).wait_send()
        pass_left(s).wait_send()

        @pl.when(s >= 1)
        def _():
            gathered(s)

        return carry

    loop(keep, finish, 0)

    def finish_mids(s, carry):
        for c in mid_copies(s):
            c.wait_send()
        return carry

    loop(nseq, finish_mids, 0)
    pack_end()
    for c in far[:4]:
        c.wait()
    far[4].wait_send()
    for c in gate_mids((before, after, opposite)):
        c.wait_recv()
    last = local(mgu, mg_out, e_sem.at[2])
    last.start()
    for c in gate_mids((chip, chip, chip)):
        c.wait_send()
    for c in exports() + [last]:
        c.wait()


def call_a(n, keep, scale, group, dim, share, x, gain, gain_mlp, wq, wk, wv, ar, agu, bqkv, wide, wo, wo_l, wo_r, wg, wu, wd, lml):
    nseq, rows, model = x.shape[0] // CORES, x.shape[1], x.shape[2]
    own = wq.shape[0]
    width = own * CORES
    rank3 = bqkv.shape[1]
    crows = CORES * ar.shape[1]
    hbm = pl.BlockSpec(memory_space=pl.ANY)
    vmem = pl.BlockSpec(memory_space=pltpu.VMEM)
    dma = pltpu.SemaphoreType.DMA
    lag = min(5, nseq)
    flops = 2 * nseq * rows * model * (3 * width + rank3)
    return pl.pallas_call(
        functools.partial(kernel_a, n, lag, keep, scale, group, dim, share),
        out_shape=[
            jax.ShapeDtypeStruct((nseq, n, rows, width), BF16),
            jax.ShapeDtypeStruct((nseq, *ar.shape[1:]), BF16),
            jax.ShapeDtypeStruct((nseq, *agu.shape[1:]), BF16),
            jax.ShapeDtypeStruct((nseq, *bqkv.shape[1:]), BF16),
            jax.ShapeDtypeStruct((n - 1, *wide.shape), BF16),
            jax.ShapeDtypeStruct((n, nseq, *wide.shape[1:]), BF16),
            jax.ShapeDtypeStruct((n - 1, *wo.shape), BF16),
            jax.ShapeDtypeStruct((n, *wo.shape), BF16),
            jax.ShapeDtypeStruct(wg.shape, BF16),
            jax.ShapeDtypeStruct(wu.shape, BF16),
            jax.ShapeDtypeStruct(wd.shape, BF16),
            jax.ShapeDtypeStruct((nseq, *lml.shape[1:]), BF16),
            jax.ShapeDtypeStruct((rows, model), BF16),
            jax.ShapeDtypeStruct((rows // n, model), BF16),
            jax.ShapeDtypeStruct((n * CORES * 2 * share, rows), BF16),
        ],
        in_specs=[hbm, vmem, vmem] + [hbm] * 14,
        out_specs=[hbm] * 15,
        scratch_shapes=[
            pltpu.VMEM((3 * width, model), BF16),
            pltpu.VMEM((PAIR, rows, model), BF16),
            pltpu.VMEM((rows, model), BF16),
            pltpu.VMEM((PAIR, crows, model), BF16),
            pltpu.VMEM((PAIR, 3, rank3, width), BF16),
            pltpu.VMEM((rows, 3 * width), BF16),
            pltpu.VMEM((PAIR, rows, width), BF16),
            pltpu.VMEM((nseq, n * crows, rows), BF16),
            pltpu.VMEM((rank3, n * crows), BF16),
            pltpu.VMEM((PAIR, model, 512), BF16),
            pltpu.VMEM((rows, model), BF16),
            pltpu.VMEM((rows, model), BF16),
            pltpu.VMEM((rows, model), BF16),
            pltpu.VMEM((rows, rank3 // 3), BF16),
            pltpu.VMEM((1, rank3 // 3, model), BF16),
            pltpu.VMEM((1, rank3 // 3, model), BF16),
            pltpu.VMEM((1, CORES * 2 * share, model), BF16),
            pltpu.VMEM((n * CORES * 2 * share, rows), BF16),
            dma((TRIPLE,)), dma((PAIR,)), dma((PAIR, 2)), dma((PAIR, 3)), dma((PAIR, 3)), dma((5,)), dma((5,)), dma((5,)), dma((5,)),
            dma((TRIPLE, nseq)), dma((TRIPLE, nseq)),
        ] + [dma((PAIR,))] * 8 + [dma((10,))] * 2 + [
            dma((PAIR,)), dma((PAIR,)), dma((PAIR,)), dma((nseq,)), dma((nseq,)), dma((nseq,)), dma((nseq,)), dma((nseq,)), dma((nseq,)),
            dma((PAIR, CORES * n + 2)), dma((1, 3, CORES * n)), dma((n,)), dma, dma((TRIPLE,)), dma((TRIPLE,)), dma((TRIPLE,)),
        ],
        compiler_params=pltpu.CompilerParams(collective_id=0, has_side_effects=True, vmem_limit_bytes=VMEM_LIMIT),
        cost_estimate=pl.CostEstimate(flops=flops, bytes_accessed=3 * x.size, transcendentals=nseq * rows * rows * width // dim),
        name="qkv_attention",
    )(x, gain, gain_mlp, wq, wk, wv, ar, agu, bqkv, wide, wo, wo_l, wo_r, wg, wu, wd, lml)


def kernel_b(n, keep, scale, rank, share,
             x, gain, att, wo, wo_l, wo_r, wo_f, wo_x, wide, wide_f, wide_x, agu, agu_oth, wg, wg_o, wu, wu_o, wd, wd_o, lml, lml_o,
             h_first, x1_first, mg_first,
             y, att_t,
             wob, gub, wdb, attv, xb, hb, mb, zb, zm, x1b, yb, in1l, in1r, in2l, in2r, in1m, in2ml, in2mr, mgu, aob, bob, agub, lgb, lub, adb, bdb, sel, mido, midg,
             wo_sem, gu_sem, wd_sem, att_sem, x_sem, lo_sem, lg_sem, bd_sem,
             s1r, s1l, s2r, s2l, ar, al, yown, fr, fl, r1l, r1r, r2l, r2r, gl, gr, hl, hr, dsend, drecv,
             t_rs, t_ls, t_rl, t_rr, t_frs, t_fls, t_fl, t_fr,
             z1s, z1r, z2rs, z2rr, z2ls, z2lr, m_send, m_recv, e_sem):
    core, chip, right, left, partner = ring(n)
    nseq, rows, model = att.shape[0], x.shape[1], x.shape[2]
    width = att.shape[3]
    ff = wg.shape[1]
    first = core * nseq
    late = nseq - keep
    crows = CORES * 2 * share
    blk = rows // n
    half = blk // 2
    before, after, opposite = lax.rem(chip + n - 1, n), lax.rem(chip + 1, n), lax.rem(chip + 2, n)
    beyond = opposite * CORES + core
    wo_t, gu_t, wd_t = wob.shape[2], gub.shape[3], wdb.shape[2]
    wo_n, gu_n, wd_n = model // wo_t, ff // gu_t, model // wd_t
    greet(right, left, partner, beyond)

    stage = OutStage(n, scale, rank, share, x, gain, (wo, wo_l, wo_r, wo_f, wo_x), (wide, wide_f, wide_x), (agu, agu_oth),
                     (wob, attv, xb, mido, aob, bob, agub), wo_sem, lo_sem)

    def gu_copies(k, own):
        at = pl.ds(pl.multiple_of(lax.rem(k, gu_n) * gu_t, gu_t), gu_t)
        slot = even(k)
        pair = (wg, wu) if own else (wg_o, wu_o)
        return [local(w.at[:, at], gub.at[slot, j], gu_sem.at[slot, j]) for j, w in enumerate(pair)]

    def gu_start(k):
        @pl.when(k < gu_n)
        def _():
            for c in gu_copies(k, True):
                c.start()

        @pl.when(k >= gu_n)
        def _():
            for c in gu_copies(k, False):
                c.start()

    def wd_copies(k):
        at = pl.ds(pl.multiple_of(k * wd_t, wd_t), wd_t)
        slot = even(k)
        return [local(w.at[:, at], wdb.at[slot, pl.ds(j * ff, ff)], wd_sem.at[slot, j]) for j, w in enumerate((wd, wd_o))]

    def att_copies(s):
        return [local(att.at[s, j], attv.at[:, pl.ds(j * width, width)], att_sem.at[j]) for j in range(n)]

    def att_start(s):
        @pl.when(s < keep)
        def _():
            start(att_copies(s))

        @pl.when(s >= keep)
        def _():
            k = jnp.maximum(s - keep, 0)
            late_in(k)
            for j, own in enumerate(att_copies(s)):
                @pl.when(chip == j)
                def _(own=own):
                    own.start()

                @pl.when(chip != j)
                def _(j=j):
                    local(att_t.at[k, j], attv.at[:, pl.ds(j * width, width)], att_sem.at[j]).start()

    def late_right(k):
        return remote(att.at[keep + k, chip], att_t.at[k, chip], t_rs.at[k], t_rl.at[k], right)

    def late_left(k):
        return remote(att.at[keep + k, chip], att_t.at[k, chip], t_ls.at[k], t_rr.at[k], left)

    def late_hops(k):
        a, b = att_t.at[k, before, head(rows // 2)], att_t.at[k, after, pl.ds(rows // 2, rows // 2)]
        return remote(a, a, t_frs.at[k], t_fl.at[k], right), remote(b, b, t_fls.at[k], t_fr.at[k], left)

    def late_pass(k):
        hop_r, hop_l = late_hops(k)
        remote(att.at[keep + k, chip], att_t.at[k, before], t_rs.at[k], t_rl.at[k], right).wait_recv()
        hop_r.start()
        remote(att.at[keep + k, chip], att_t.at[k, after], t_ls.at[k], t_rr.at[k], left).wait_recv()
        hop_l.start()

    def late_in(k):
        a, b = att_t.at[k, opposite, head(rows // 2)], att_t.at[k, opposite, pl.ds(rows // 2, rows // 2)]
        remote(a, a, t_frs.at[k], t_fl.at[k], right).wait_recv()
        remote(b, b, t_fls.at[k], t_fr.at[k], left).wait_recv()

    def x_copy(s):
        return local(x.at[first + s], xb, x_sem)

    def lora_o(s):
        return stage.lora(s, even(s))

    def lora_m(s):
        slot, out = even(s), []
        for j, (src, k) in enumerate(((lml, first + s), (lml_o, s))):
            at = pl.ds(j * ff, ff)
            out.append(local(src.at[k, head(rank)], lgb.at[slot, head(rank), at], lg_sem.at[slot, 3 * j]))
            out.append(local(src.at[k, pl.ds(rank, rank)], lub.at[slot, pl.ds(rank, rank), at], lg_sem.at[slot, 3 * j + 1]))
            out.append(local(src.at[k, pl.ds(2 * rank, rank)], adb.at[slot, head(rank), at], lg_sem.at[slot, 3 * j + 2]))
        return out

    def start(copies):
        for c in copies:
            c.start()

    def wait(copies):
        for c in copies:
            c.wait()

    def rows_of(j, size=blk, shift=0):
        return pl.ds(pl.multiple_of(j * blk + shift, size), size)

    def rs1_right(s):
        return remote(zb.at[third(s), rows_of(opposite, half)], in1l.at[third(s)], s1r.at[s], r1l.at[s], right)

    def rs1_left(s):
        return remote(zb.at[third(s), rows_of(opposite, half, half)], in1r.at[third(s)], s1l.at[s], r1r.at[s], left)

    def rs2_right(s):
        return remote(zb.at[third(s), rows_of(after)], in2l.at[third(s)], s2r.at[s], r2l.at[s], right)

    def rs2_left(s):
        return remote(zb.at[third(s), rows_of(before)], in2r.at[third(s)], s2l.at[s], r2r.at[s], left)

    def ag1_right(s):
        return remote(yb.at[even(s)], y.at[first + s, rows_of(chip)], ar.at[s], gl.at[s], right)

    def ag1_left(s):
        return remote(yb.at[even(s)], y.at[first + s, rows_of(chip)], al.at[s], gr.at[s], left)

    def ag1_own(s):
        return local(yb.at[even(s)], y.at[first + s, rows_of(chip)], yown.at[s])

    def ag2_right(s, block):
        part = y.at[first + s, rows_of(block, half)]
        return remote(part, part, fr.at[s], hl.at[s], right)

    def ag2_left(s, block):
        part = y.at[first + s, rows_of(block, half, half)]
        return remote(part, part, fl.at[s], hr.at[s], left)

    def across(s, k, block):
        part = y.at[first + s, rows_of(block)]
        return remote(yb.at[even(s)] if k == 0 else part, part, dsend.at[k, s], drecv.at[k, s], partner)

    def across_in(s, k):
        there = y.at[(1 - core) * nseq + s, rows_of((chip, before, after, opposite)[k])]
        return remote(there, there, dsend.at[k, s], drecv.at[k, s], partner)

    def lanes_of(j):
        return pl.ds(pl.multiple_of(j * blk, blk), blk)

    def zm1(s):
        return remote(zm.at[third(s), :, lanes_of(opposite)], in1m.at[third(s)], z1s.at[s], z1r.at[s], right)

    def zm2_right(s):
        return remote(zm.at[third(s), :, lanes_of(after)], in2ml.at[third(s)], z2rs.at[s], z2rr.at[s], right)

    def zm2_left(s):
        return remote(zm.at[third(s), :, lanes_of(before)], in2mr.at[third(s)], z2ls.at[s], z2lr.at[s], left)

    def rank_rows(j):
        return pl.ds(pl.multiple_of(j * crows, crows), crows)

    def mid_copies(s, froms):
        return [remote(mgu.at[s, rank_rows(j)], mgu.at[s, rank_rows(j)], m_send.at[k, s], m_recv.at[k, s], to)
                for k, (j, to) in enumerate(zip(froms, (right, left, beyond)))]

    def do_rs2(s):
        slot = third(s)
        zm1(s).wait_recv()
        at = lanes_of(after)
        zm[slot, :, at] = (zm[slot, :, at].astype(F32) + in1m[slot].astype(F32)).astype(BF16)
        zm2_right(s).start()
        zm2_left(s).start()
        rs1_right(s).wait_recv()
        at = rows_of(after, half)
        zb[slot, at, :] = (zb[slot, at, :].astype(F32) + in1l[slot].astype(F32)).astype(BF16)
        rs2_right(s).start()
        rs1_left(s).wait_recv()
        at = rows_of(before, half, half)
        zb[slot, at, :] = (zb[slot, at, :].astype(F32) + in1r[slot].astype(F32)).astype(BF16)
        rs2_left(s).start()

    def do_rs3(s):
        slot, yslot = third(s), even(s)

        @pl.when(s >= 2)
        def _():
            ag1_right(s - 2).wait_send()
            ag1_left(s - 2).wait_send()
            ag1_own(s - 2).wait()
            across(s - 2, 0, chip).wait_send()

        rs2_right(s).wait_recv()
        rs2_left(s).wait_recv()
        mine = zb.at[slot, rows_of(chip)]
        zm2_right(s).wait_recv()
        zm2_left(s).wait_recv()
        mid = zm[slot, :, lanes_of(chip)].astype(F32) + in2ml[slot].astype(F32) + in2mr[slot].astype(F32)
        mid = mid.T.astype(BF16)

        def piece(k, carry):
            at = pl.ds(pl.multiple_of(k * wo_t, wo_t), wo_t)
            z = mine[:, at].astype(F32) + in2l[slot, :, at].astype(F32) + in2r[slot, :, at].astype(F32)
            z = z + scale * dot(mid, bdb[s, :, at])
            yb[yslot, :, at] = (x1b[lax.rem(s, 4), :, at].astype(F32) + z).astype(BF16)
            return carry

        loop(wo_n, piece, 0)
        ag1_right(s).start()
        ag1_left(s).start()
        ag1_own(s).start()
        across(s, 0, chip).start()

    def do_ag2(s):
        remote(yb.at[0], y.at[first + s, rows_of(before)], ar.at[s], gl.at[s], right).wait_recv()
        ag2_right(s, before).start()
        across(s, 1, before).start()
        remote(yb.at[0], y.at[first + s, rows_of(after)], al.at[s], gr.at[s], left).wait_recv()
        ag2_left(s, after).start()
        across(s, 2, after).start()

    def do_across(s):
        ag2_right(s, opposite).wait_recv()
        ag2_left(s, opposite).wait_recv()
        across(s, 3, opposite).start()

    def when(cond, f, s):
        @pl.when(cond)
        def _():
            f(s)

    for k in range(min(late, 2)):
        late_right(k).start()
        late_left(k).start()
    bd_copies = [local(stage.share_of((wide, wide_f, wide_x), cross, j).at[pl.ds(0 if cross else first, nseq), pl.ds(2 * rank, rank)],
                       bdb.at[:, :, stage.cols(d)], bd_sem.at[4 * cross + j]) for d, cross, j in stage.shares]
    done = [local(h_first, hb.at[0], e_sem.at[0]), local(x1_first, x1b.at[0], e_sem.at[1]), local(mg_first, mgu.at[0], e_sem.at[2])]
    start(done)
    start(bd_copies)
    sel[...] = pick(sel.shape, share, rank, 2, 1)
    for k in range(2):
        start(stage.wo_copies(k))
        start(gu_copies(k, True))
        start(wd_copies(k))
    att_start(jnp.int32(1))
    x_copy(1).start()
    start(lora_o(1))
    lgb[...] = jnp.zeros_like(lgb)
    lub[...] = jnp.zeros_like(lub)
    start(lora_m(0))
    wait(bd_copies)
    wait(done)

    def out_proj(s):
        slot = even(s)
        wait(lora_o(s))
        wait(att_copies(s))
        x_copy(s).wait()
        stage.first_product(slot)
        stage.tiles(slot, 0, wo_n // 2, s + 1 < nseq)

    def out_proj_end(s):
        slot = even(s)
        stage.tiles(slot, wo_n // 2, wo_n, s + 1 < nseq)
        stage.norm(slot, hb.at[slot], mgu.at[s, rank_rows(chip)])
        start(mid_copies(s, (chip, chip, chip)))
        for k in range(2, late):
            @pl.when(s == k - 1)
            def _(k=k):
                late_right(k).start()
                late_left(k).start()

        x1b[lax.rem(s, 4)] = xb[rows_of(chip), :]

        @pl.when(s + 1 < nseq)
        def _():
            start(lora_o(s + 1))
            att_start(s + 1)
            x_copy(s + 1).start()

    def gate_up(s):
        slot = even(s)
        @pl.when(s >= 1)
        def _():
            for c in mid_copies(s, (before, after, opposite)):
                c.wait_recv()

        midg[...] = dot(sel[...], mgu[s]).T.astype(BF16)
        wait(lora_m(s))
        gate_tiles(s, 0, gu_n)

    def gate_tiles(s, lo, hi):
        slot = even(s)
        h = hb.at[slot]
        mid = midg[...]

        def tile(k, carry):
            at = pl.ds(pl.multiple_of(k * gu_t, gu_t), gu_t)
            wait(gu_copies(k, True))
            g = dot(h[...], gub[even(k), 0]) + scale * dot(mid, lgb[slot, :, at])
            u = dot(h[...], gub[even(k), 1]) + scale * dot(mid, lub[slot, :, at])
            g = g.astype(BF16).astype(F32)
            u = u.astype(BF16).astype(F32)
            mb[:, at] = (jax.nn.silu(g) * u).astype(BF16)

            @pl.when((k + 2 < 2 * gu_n) | (s + 1 < nseq))
            def _():
                gu_start(lax.rem(k + 2, 2 * gu_n))

            return carry

        lax.fori_loop(lo, hi, tile, 0)

    def gate_up_end(s):
        gate_tiles(s, gu_n, 2 * gu_n)

        @pl.when(s + 1 < nseq)
        def _():
            start(lora_m(s + 1))

    def down(s):
        slot = third(s)

        @pl.when(s >= 3)
        def _():
            rs1_right(s - 3).wait_send()
            rs1_left(s - 3).wait_send()
            rs2_right(s - 3).wait_send()
            rs2_left(s - 3).wait_send()
            zm1(s - 3).wait_send()
            zm2_right(s - 3).wait_send()
            zm2_left(s - 3).wait_send()

        zm[slot] = dot_nt(adb[even(s)], mb[...]).astype(BF16)

        def tile(k, carry):
            at = pl.ds(pl.multiple_of(k * wd_t, wd_t), wd_t)
            wait(wd_copies(k))
            zb[slot, :, at] = dot(mb[...], wdb[even(k)]).astype(BF16)

            @pl.when((k + 2 < wd_n) | (s + 1 < nseq))
            def _():
                start(wd_copies(lax.rem(k + 2, wd_n)))

            return carry

        loop(wd_n, tile, 0)
        zm1(s).start()
        rs1_right(s).start()
        rs1_left(s).start()

    def step(f, t, lag, ahead=0):
        s = t - lag + ahead
        when((s >= 0) & (s < nseq), f, s)

    def body(t, carry):
        step(out_proj, t, 0, 1)
        step(do_rs3, t, 2)
        step(out_proj_end, t, 0, 1)
        for k, stages in enumerate(((), (gate_up, do_rs2, do_ag2, gate_up_end), (down,))):
            for f in stages:
                step(f, t, {do_rs2: 1, do_ag2: 2}.get(f, 0))
            if k < late:
                when(t == 0, lambda _, k=k: late_pass(k), t)
        step(do_across, t, 3)
        return carry

    loop(nseq + 3, body, 0)

    for s in range(max(nseq - 3, 0), nseq):
        rs1_right(s).wait_send()
        rs1_left(s).wait_send()
        rs2_right(s).wait_send()
        rs2_left(s).wait_send()
        zm1(s).wait_send()
        zm2_right(s).wait_send()
        zm2_left(s).wait_send()
    for s in range(max(nseq - 2, 0), nseq):
        ag1_right(s).wait_send()
        ag1_left(s).wait_send()
        ag1_own(s).wait()
        across(s, 0, chip).wait_send()

    def finish(s, carry):
        @pl.when(s >= 1)
        def _():
            for c in mid_copies(s, (chip, chip, chip)):
                c.wait_send()

        ag2_right(s, before).wait_send()
        ag2_left(s, after).wait_send()
        for k, block in ((1, before), (2, after), (3, opposite)):
            across(s, k, block).wait_send()
        for k in range(4):
            across_in(s, k).wait_recv()
        return carry

    loop(nseq, finish, 0)
    for k in range(late):
        late_right(k).wait_send()
        late_left(k).wait_send()
        for hop in late_hops(k):
            hop.wait_send()


def call_b(n, keep, scale, rank, share, x, gain, att, wo, wo_l, wo_r, wo_f, wo_x, wide, wide_f, wide_x, agu, agu_oth, wg, wg_o, wu, wu_o, wd, wd_o, lml, lml_o, h_first, x1_first, mg_first):
    nseq, rows, model, ff = att.shape[0], x.shape[1], x.shape[2], wg.shape[1]
    hbm = pl.BlockSpec(memory_space=pl.ANY)
    vmem = pl.BlockSpec(memory_space=pltpu.VMEM)
    dma = pltpu.SemaphoreType.DMA
    blk = rows // n
    ndev = CORES * n
    tile = 512
    flops = 2 * nseq * rows * (model * model + 3 * model * ff * CORES)
    return pl.pallas_call(
        functools.partial(kernel_b, n, keep, scale, rank, share),
        out_shape=[jax.ShapeDtypeStruct(x.shape, BF16), jax.ShapeDtypeStruct((nseq - keep, *att.shape[1:]), BF16)],
        in_specs=[hbm, vmem] + [hbm] * 22,
        out_specs=[hbm] * 2,
        scratch_shapes=[
            pltpu.VMEM((PAIR, model, tile), BF16),
            pltpu.VMEM((PAIR, 2, model, tile // 2), BF16),
            pltpu.VMEM((PAIR, CORES * ff, tile), BF16),
            pltpu.VMEM((rows, model), BF16),
            pltpu.VMEM((rows, model), BF16),
            pltpu.VMEM((PAIR, rows, model), BF16),
            pltpu.VMEM((rows, CORES * ff), BF16),
            pltpu.VMEM((TRIPLE, rows, model), BF16),
            pltpu.VMEM((TRIPLE, rank, rows), BF16),
            pltpu.VMEM((QUAD, blk, model), BF16),
            pltpu.VMEM((PAIR, blk, model), BF16),
            pltpu.VMEM((TRIPLE, blk // 2, model), BF16),
            pltpu.VMEM((TRIPLE, blk // 2, model), BF16),
            pltpu.VMEM((TRIPLE, blk, model), BF16),
            pltpu.VMEM((TRIPLE, blk, model), BF16),
            pltpu.VMEM((TRIPLE, rank, blk), BF16),
            pltpu.VMEM((TRIPLE, rank, blk), BF16),
            pltpu.VMEM((TRIPLE, rank, blk), BF16),
            pltpu.VMEM((nseq, n * CORES * 2 * share, rows), BF16),
            pltpu.VMEM((PAIR, rank, model), BF16),
            pltpu.VMEM((PAIR, rank, model), BF16),
            pltpu.VMEM((PAIR, CORES * 2 * share, model), BF16),
            pltpu.VMEM((PAIR, 2 * rank, CORES * ff), BF16),
            pltpu.VMEM((PAIR, 2 * rank, CORES * ff), BF16),
            pltpu.VMEM((PAIR, rank, CORES * ff), BF16),
            pltpu.VMEM((nseq, rank, model), BF16),
            pltpu.VMEM((2 * rank, 2 * rank), BF16),
            pltpu.VMEM((rows, rank), BF16),
            pltpu.VMEM((rows, 2 * rank), BF16),
            dma((PAIR, ndev + 2)), dma((PAIR, 2)), dma((PAIR, 2)), dma((n,)), dma, dma((PAIR, 3, ndev)), dma((PAIR, 6)), dma((ndev,)),
        ] + [dma((nseq,))] * 17 + [dma((QUAD, nseq))] * 2 + [dma((nseq - keep,))] * 8 + [dma((nseq,))] * 6 + [dma((TRIPLE, nseq))] * 2 + [dma((TRIPLE,))],
        compiler_params=pltpu.CompilerParams(collective_id=1, has_side_effects=True, vmem_limit_bytes=VMEM_LIMIT),
        cost_estimate=pl.CostEstimate(flops=flops, bytes_accessed=4 * x.size, transcendentals=0),
        name="out_mlp",
    )(x, gain, att, wo, wo_l, wo_r, wo_f, wo_x, wide, wide_f, wide_x, agu, agu_oth, wg, wg_o, wu, wu_o, wd, wd_o, lml, lml_o, h_first, x1_first, mg_first)[0]


def solution(mesh):
    n = mesh.shape["tp"] // CORES
    act_spec = P("dp", N, N)
    w_head, w_out, w_col, w_row = P(N, "tp", N), P("tp", N, N), P(N, "tp"), P("tp", N)
    a_rank, b_head, b_col = P(N, N, "tp"), P(N, N, "tp", N), P(N, N, "tp")
    a_head, a_row = P(N, "tp", N, N), P(N, "tp", N)
    in_specs = (act_spec, P("dp"), P(N), P(N), w_head, w_head, w_head, w_out, w_col, w_col, w_row,
                a_rank, b_head, a_rank, b_head, a_rank, b_head, a_head, b_col, a_rank, b_col, a_rank, b_col, a_row, b_col)

    def local_layer(x_in, adapter_ids, gain_attn, gain_mlp, w_q, w_k, w_v, w_o, w_gate, w_up, w_down,
                    a_q, b_q, a_k, b_k, a_v, b_v, a_o, b_o, a_gate, b_gate, a_up, b_up, a_down, b_down):
        nseq, model = x_in.shape[0], x_in.shape[2]
        rank, dim = b_q.shape[1], w_q.shape[2]
        own = w_q.shape[1] * dim
        scale = LORA_ALPHA / rank
        share = a_q.shape[2]
        group = math.lcm(dim, 128) // dim
        keep = max(nseq // CORES - 3, 1)

        def take(*stacks):
            return jnp.take(jnp.concatenate(stacks, axis=1), adapter_ids, axis=0, mode="clip")

        def turn(stack):
            return jnp.swapaxes(stack, 1, 2)

        wo = w_o.reshape(own, model)
        ndev = n * CORES
        upper = wo[:own // 2]
        wo_l = lax.ppermute(upper, "tp", [(d, (d + CORES) % ndev) for d in range(ndev)])
        wo_r = lax.ppermute(upper, "tp", [((d + CORES) % ndev, d) for d in range(ndev)])
        ar = take(turn(a_q), turn(a_k), turn(a_v), jnp.zeros((a_q.shape[0], share, model), BF16))
        agu = take(turn(a_gate), turn(a_up))
        bqkv = take(*[b.reshape(-1, rank, own) for b in (b_q, b_k, b_v)])
        wide = take(turn(a_o.reshape(-1, own, rank)), b_o, b_down)
        lml = take(b_gate, b_up, turn(a_down))
        flat = [jnp.transpose(w, (1, 2, 0)).reshape(own, model) for w in (w_q, w_k, w_v)]
        att, _, agu_oth, _, wide_f, wide_x, wo_f, wo_x, wg_o, wu_o, wd_o, lml_o, *head = call_a(
            n, keep, scale, group, dim, share, x_in, gain_attn.reshape(1, model), gain_mlp.reshape(1, model), *flat, ar, agu, bqkv, wide,
            wo, wo_l, wo_r, w_gate, w_up, w_down, lml)
        return call_b(n, keep, scale, rank, share, x_in, gain_mlp.reshape(1, model), att, wo, wo_l, wo_r, wo_f, wo_x, wide, wide_f, wide_x,
                      agu, agu_oth, w_gate, wg_o, w_up, wu_o, w_down, wd_o, lml, lml_o, *head)

    return jax.shard_map(local_layer, mesh=mesh, in_specs=in_specs, out_specs=act_spec, check_vma=False)
```

```python
import functools
import math

import jax
import jax.numpy as jnp
from jax import lax
from jax.experimental import pallas as pl
from jax.experimental.pallas import tpu as pltpu
from jax.sharding import PartitionSpec as P

LORA_ALPHA = 16
RMS_EPS = 1e-5
CORES = 2
MESH = pl.DeviceIdType.MESH
F32, BF16 = jnp.float32, jnp.bfloat16
NT = (((1,), (1,)), ((), ()))
VMEM_LIMIT = 67_000_000
PAIR, TRIPLE, QUAD = 2, 3, 4
LANES = 128
N = None


def even(k):
    return lax.rem(k, PAIR)


def third(k):
    return lax.rem(k, TRIPLE)


def head(size):
    return pl.ds(0, size)


def loop(count, body, start):
    return lax.fori_loop(0, count, body, start)


def dot(a, b):
    return jnp.dot(a, b, preferred_element_type=F32)


def dot_nt(a, b):
    return lax.dot_general(a, b, NT, preferred_element_type=F32)


def ring(n):
    me = lax.axis_index("tp")
    core, chip = lax.rem(me, CORES), lax.div(me, CORES)
    right = lax.rem(chip + 1, n) * CORES + core
    left = lax.rem(chip + n - 1, n) * CORES + core
    return core, chip, right, left, chip * CORES + 1 - core


def greet(*others):
    barrier = pltpu.get_barrier_semaphore()
    for other in others:
        pl.semaphore_signal(barrier, inc=1, device_id={"tp": other}, device_id_type=MESH)
    pl.semaphore_wait(barrier, len(others))


def remote(src, dst, send, recv, to):
    return pltpu.make_async_remote_copy(src_ref=src, dst_ref=dst, send_sem=send, recv_sem=recv, device_id={"tp": to},
                                        device_id_type=MESH)


def local(src, dst, sem):
    return pltpu.make_async_copy(src, dst, sem)


def rms_rows(src, dst, gain, rows, step):
    def chunk(k, carry):
        at = pl.ds(pl.multiple_of(k * step, step), step)
        v = src[at, :].astype(F32)
        inv = lax.rsqrt(jnp.mean(v * v, axis=-1, keepdims=True) + RMS_EPS)
        dst[at, :] = (v * inv * gain[...]).astype(BF16)
        return carry

    loop(rows // step, chunk, 0)


def head_windows(group, dim):
    out = []
    for h in range(group):
        lo, hi = h * dim, (h + 1) * dim
        start, stop = lo // 128 * 128, -(-hi // 128) * 128
        out.append((start, stop, lo - start, hi - start))
    return out


def attend(qkv, out, width, group, dim, qblock):
    seq = qkv.shape[0]
    lanes = group * dim

    def one_group(g, carry):
        base = pl.multiple_of(g * lanes, 128)
        for qb in range(seq // qblock):
            rows, keys = pl.ds(qb * qblock, qblock), (qb + 1) * qblock
            acc = [None] * (lanes // 128)
            mask = (lax.broadcasted_iota(jnp.int32, (qblock, keys), 0) + qb * qblock
                    >= lax.broadcasted_iota(jnp.int32, (qblock, keys), 1))
            for start, stop, lo, hi in head_windows(group, dim):
                size = stop - start
                lane_q = lax.broadcasted_iota(jnp.int32, (qblock, size), 1)
                lane_k = lax.broadcasted_iota(jnp.int32, (keys, size), 1)
                q = qkv[rows, pl.ds(base + start, size)]
                k = qkv[head(keys), pl.ds(width + base + start, size)]
                v = qkv[head(keys), pl.ds(2 * width + base + start, size)]
                q = jnp.where((lane_q >= lo) & (lane_q < hi), q, jnp.zeros_like(q))
                v = jnp.where((lane_k >= lo) & (lane_k < hi), v, jnp.zeros_like(v))
                scores = jnp.where(mask, dot_nt(q, k) * dim ** -0.5, -jnp.inf)
                top = jnp.max(scores, axis=-1, keepdims=True)
                e = jnp.exp(scores - top)
                prob = (e / jnp.sum(e, axis=-1, keepdims=True)).astype(BF16)
                o = dot(prob, v)
                for t in range(size // 128):
                    piece = o[:, t * 128:(t + 1) * 128]
                    j = start // 128 + t
                    acc[j] = piece if acc[j] is None else acc[j] + piece
            for j, piece in enumerate(acc):
                out[rows, pl.ds(base + j * 128, 128)] = piece.astype(BF16)
        return carry

    loop(width // lanes, one_group, 0)


def pick(shape, share, ranks, slots, axis):
    i = lax.broadcasted_iota(jnp.int32, shape, axis)
    t = lax.broadcasted_iota(jnp.int32, shape, 1 - axis)
    dev, slot, r = i // (slots * share), (i // share) % slots, i % share
    return jnp.where(t == slot * ranks + dev * share + r, 1.0, 0.0).astype(BF16)


class OutStage:
    def __init__(self, n, scale, rank, share, x, gain, wo_refs, wide_refs, agu_refs, bufs, wo_sem, lo_sem):
        self.core, self.chip, *_ = ring(n)
        self.before, self.after = lax.rem(self.chip + n - 1, n), lax.rem(self.chip + 1, n)
        self.opposite = lax.rem(self.chip + 2, n)
        self.scale, self.rank, self.share, self.x, self.gain = scale, rank, share, x, gain
        self.wide_refs, self.agu_refs, self.bufs = wide_refs, agu_refs, bufs
        self.wo_sem, self.lo_sem = wo_sem, lo_sem
        self.rows, self.first = x.shape[1], self.core * (x.shape[0] // CORES)
        wo, wo_p, wo_f, wo_x = wo_refs
        deep = wo.shape[0]
        self.width = wide_refs[0].shape[2]
        self.tile_w = bufs[0].shape[2]
        self.tiles_n = x.shape[2] // self.tile_w
        chips = (self.chip, self.before, self.after, self.opposite)
        self.shares = [(CORES * c + self.core, 0, j) for j, c in enumerate(chips)]
        self.shares += [(CORES * c + 1 - self.core, 1, j) for j, c in enumerate(chips)]
        self.wo_shares = []
        for d, cross, j in self.shares:
            src = self.share_of((wo, wo_f, wo_x), cross, j)
            early = wo_p if not cross and j in (1, 2) else src
            both = (early, src) if j == 1 else (src, early)
            self.wo_shares.append((both, pl.ds(pl.multiple_of(d * deep, deep), deep)))

    @staticmethod
    def share_of(refs, cross, j):
        return refs[2].at[j] if cross else refs[0] if j == 0 else refs[1].at[j - 1]

    def cols(self, d):
        return pl.ds(pl.multiple_of(d * self.width, self.width), self.width)

    def wo_copies(self, k, core=0):
        wob = self.bufs[0]
        at, slot = pl.ds(pl.multiple_of(k * self.tile_w, self.tile_w), self.tile_w), even(k)
        return [local(both[core].at[:, at], wob.at[slot, rows_at], self.wo_sem.at[slot, j])
                for j, (both, rows_at) in enumerate(self.wo_shares)]

    def wo_start(self, k):
        for core in range(CORES):
            @pl.when(self.core == core)
            def _(core=core):
                for c in self.wo_copies(k, core):
                    c.start()

    def lora(self, s, slot):
        _, _, _, _, aob, bob, agub = self.bufs
        rank, out = self.rank, []
        for d, cross, j in self.shares:
            src = self.share_of(self.wide_refs, cross, j).at[s if cross else self.first + s]
            out.append(local(src.at[head(rank)], aob.at[slot, :, self.cols(d)], self.lo_sem.at[slot, 0, 4 * cross + j]))
            out.append(local(src.at[pl.ds(rank, rank)], bob.at[slot, :, self.cols(d)], self.lo_sem.at[slot, 1, 4 * cross + j]))
        for i, (j, src, k) in enumerate(((self.core, self.agu_refs[0], self.first + s), (1 - self.core, self.agu_refs[1], s))):
            rows_at = pl.ds(pl.multiple_of(j * 2 * self.share, 2 * self.share), 2 * self.share)
            out.append(local(src.at[k], agub.at[slot, rows_at], self.lo_sem.at[slot, 2, i]))
        return out

    def first_product(self, slot):
        _, attv, _, mido, aob, _, _ = self.bufs
        mido[...] = dot_nt(attv[...], aob[slot]).astype(BF16)

    def tiles(self, slot, lo, hi, more):
        wob, attv, xb, mido, _, bob, _ = self.bufs
        mid = mido[...]

        def tile(k, carry):
            at = pl.ds(pl.multiple_of(k * self.tile_w, self.tile_w), self.tile_w)
            for c in self.wo_copies(k):
                c.wait()
            z = dot(attv[...], wob[even(k)]) + self.scale * dot(mid, bob[slot, :, at])
            xb[:, at] = (xb[:, at].astype(F32) + z).astype(BF16)

            @pl.when((k + 2 < self.tiles_n) | more)
            def _():
                self.wo_start(lax.rem(k + 2, self.tiles_n))

            return carry

        lax.fori_loop(lo, hi, tile, 0)

    def norm(self, slot, h, mid_rows):
        _, _, xb, _, _, _, agub = self.bufs
        rms_rows(xb, h, self.gain, self.rows, 64)
        mid_rows[...] = dot_nt(agub[slot], h[...]).astype(BF16)


def kernel_a(n, lag, keep, scale, group, dim, share,
             x, gain, gain_mlp, wq, wk, wv, ar, agu, bqkv, wide, wo, wo_p, wg, wu, wd, lml,
             att, ar_oth, agu_oth, b_oth, wide_f, wide_x, wo_f, wo_x, wg_o, wu_o, wd_o, lml_o, h_out, x1_out, mg_out,
             wbuf, xbuf, hbuf, abuf, bbuf, qkv, attb, mids, sel, wob, attv, xb, hb, mido, aob, bob, agub, mgu,
             w_sem, x_sem, a_sem, bo_sem, bp_sem, d_send, d_recv, o_send, o_recv, m_send, m_recv,
             pr_send, pl_send, prl_recv, prr_recv, pfr_send, pfl_send, pfl_recv, pfr_recv, pp_send, pp_recv,
             r_send, l_send, own_sem, rl_recv, rr_recv, fr_send, fl_send, fl_recv, fr_recv,
             wo_sem, lo_sem, att_sem, xo_sem, g_send, g_recv, e_sem):
    core, chip, right, left, partner = ring(n)
    before, after, opposite = lax.rem(chip + n - 1, n), lax.rem(chip + 1, n), lax.rem(chip + 2, n)
    across = opposite * CORES + core
    nseq, rows, own = x.shape[0] // CORES, x.shape[1], wq.shape[0]
    width = own * CORES
    first = core * nseq
    rank = bqkv.shape[1] // 3
    arows = ar.shape[1]
    crows = CORES * arows
    greet(right, left, partner, across)

    theirs, mine_at = pl.ds((1 - core) * nseq, nseq), pl.ds(first, nseq)
    near = [remote(ar.at[theirs], ar_oth, d_send.at[4], d_recv.at[4], partner)]
    near += [remote(w, wbuf.at[pl.ds(p * width + core * own, own)], d_send.at[p], d_recv.at[p], partner)
             for p, w in enumerate((wq, wk, wv))]
    near.append(remote(bqkv.at[theirs], b_oth, d_send.at[3], d_recv.at[3], partner))
    far = [remote(src, dst, o_send.at[k], o_recv.at[k], partner)
           for k, (src, dst) in enumerate(((lml.at[theirs], lml_o), (wg, wg_o), (wu, wu_o), (wd, wd_o),
                                     (agu.at[theirs], agu_oth)))]
    mine = [local(w, wbuf.at[pl.ds(p * width + core * own, own)], w_sem.at[p]) for p, w in enumerate((wq, wk, wv))]

    to_right, to_left = (right, pr_send, prl_recv, pfr_send, pfl_recv), (left, pl_send, prr_recv, pfl_send, pfr_recv)

    def by_core(f):
        for c in range(CORES):
            @pl.when(core == c)
            def _(c=c):
                f(c)

    def pack_first(k, way):
        to, send, recv, _, _ = (to_right, to_left)[way]
        src, dst = ((wide, wide_f), (wo, wo_f))[k]
        return remote(src, dst.at[way], send.at[k], recv.at[k], to)

    def pack_second(k, way, early=False):
        to, _, _, send, recv = (to_right, to_left)[way]
        dst = (wide_f, wo_f)[k]
        part_n = dst.shape[1] // 2
        part = pl.ds(way * part_n, part_n)
        return remote(wo_p.at[part] if early else dst.at[way, part], dst.at[2, part], send.at[k], recv.at[k], to)

    def wide_push(j):
        src = wide if j == 0 else wide_f.at[j - 1]
        return remote(src.at[theirs], wide_x.at[j], pp_send.at[j], pp_recv.at[j], partner)

    def wo_push(j, early=False):
        src = wo if j == 0 else wo_p if early else wo_f.at[j - 1]
        return remote(src, wo_x.at[j], pp_send.at[QUAD + j], pp_recv.at[QUAD + j], partner)

    def wo_first(c):
        pack_first(1, 1 - c).start()
        wo_push(0).start()
        wo_push(1 + c, True).start()

    def wo_next(c):
        pack_first(1, 1 - c).wait_recv()
        pack_second(1, 1 - c).start()
        wo_push(2 - c).start()

    def pack_start(k):
        if k == 1:
            by_core(wo_first)
            return
        for way in range(PAIR):
            pack_first(k, way).start()
        wide_push(0).start()

    def pack_pass(k):
        if k == 1:
            by_core(wo_next)
            return
        for way in range(PAIR):
            pack_first(k, way).wait_recv()
            pack_second(k, way).start()
            wide_push(way + 1).start()

    def pack_across(k):
        for way in range(PAIR):
            pack_second(k, way).wait_recv()
        (wide_push if k == 0 else wo_push)(TRIPLE).start()

    def wo_ready():
        for j in range(QUAD):
            wide_push(j).wait_recv()
            wo_push(j).wait_recv()
        far[QUAD].wait_recv()

    def pack_end():
        for way in range(PAIR):
            pack_first(0, way).wait_send()
            for k in range(PAIR):
                pack_second(k, way).wait_send()
        by_core(lambda c: pack_first(1, 1 - c).wait_send())
        for j in range(QUAD):
            wide_push(j).wait_send()
            wo_push(j).wait_send()

    def x_copy(g):
        return local(x.at[first + lax.rem(g, nseq)], xbuf.at[even(g)], x_sem.at[even(g)])

    def a_copies(s):
        slot = even(s)
        own_at = pl.ds(pl.multiple_of(core * arows, arows), arows)
        oth_at = pl.ds(pl.multiple_of((1 - core) * arows, arows), arows)
        return [local(ar.at[first + s], abuf.at[slot, own_at], a_sem.at[slot, 0]),
                local(ar_oth.at[s], abuf.at[slot, oth_at], a_sem.at[slot, 1])]

    def b_copies(s):
        slot, out = even(s), []
        for p in range(3):
            part = pl.ds(p * rank, rank)
            own_at = pl.ds(pl.multiple_of(core * own, 128), own)
            oth_at = pl.ds(pl.multiple_of((1 - core) * own, 128), own)
            out.append(local(bqkv.at[first + s, part], bbuf.at[slot, p, part, own_at], bo_sem.at[slot, p]))
            out.append(local(b_oth.at[s, part], bbuf.at[slot, p, part, oth_at], bp_sem.at[slot, p]))
        return out

    near[0].start()
    pack_start(0)
    for c in near[1:] + mine:
        c.start()
    x_copy(0).start()
    bbuf[...] = jnp.zeros_like(bbuf)
    sel[...] = pick(sel.shape, share, rank, arows // share, 1)
    near[0].wait()
    for c in a_copies(0):
        c.start()

    def rank_rows(j):
        return pl.ds(pl.multiple_of(j * crows, crows), crows)

    def mid_copies(s, source=None):
        froms = (chip, chip, chip) if source is None else source
        return [remote(mids.at[s, rank_rows(j)], mids.at[s, rank_rows(j)], m_send.at[k, s], m_recv.at[k, s], to)
                for k, (j, to) in enumerate(zip(froms, (right, left, across)))]

    def first_product(s, carry):
        slot = even(s)
        x_copy(s + 1).start()

        @pl.when(s + 1 < nseq)
        def _():
            for c in a_copies(s + 1):
                c.start()

        @pl.when(s == nseq // 2)
        def _():
            pack_start(1)

        x_copy(s).wait()
        rms_rows(xbuf.at[slot], hbuf, gain, rows, 32)
        for c in a_copies(s):
            c.wait()
        mids[s, rank_rows(chip), :] = dot_nt(abuf[slot], hbuf[...]).astype(BF16)
        for c in mid_copies(s):
            c.start()
        return carry

    loop(nseq, first_product, 0)
    by_core(lambda c: pack_second(1, c, True).start())
    for c in near[1:]:
        c.wait()
    for c in b_copies(0):
        c.start()
    for c in far:
        c.start()
    for c in mine:
        c.wait()

    half = rows // 2

    def out_right(s):
        return remote(attb.at[even(s)], att.at[s, chip], r_send.at[even(s)], rl_recv.at[s], right)

    def out_left(s):
        return remote(attb.at[even(s)], att.at[s, chip], l_send.at[even(s)], rr_recv.at[s], left)

    def out_own(s):
        return local(attb.at[even(s)], att.at[s, chip], own_sem.at[even(s)])

    def in_left(s):
        return remote(attb.at[0], att.at[s, before], r_send.at[0], rl_recv.at[s], right)

    def in_right(s):
        return remote(attb.at[0], att.at[s, after], l_send.at[0], rr_recv.at[s], left)

    def pass_right(s):
        part = att.at[s, before, head(half)]
        return remote(part, part, fr_send.at[s], fl_recv.at[s], right)

    def pass_left(s):
        part = att.at[s, after, pl.ds(half, half)]
        return remote(part, part, fl_send.at[s], fr_recv.at[s], left)

    def forward(s):
        in_left(s).wait_recv()
        pass_right(s).start()
        in_right(s).wait_recv()
        pass_left(s).start()

    def gathered(s):
        got_a, got_b = att.at[s, opposite, head(half)], att.at[s, opposite, pl.ds(half, half)]
        remote(got_a, got_a, fr_send.at[s], fl_recv.at[s], right).wait_recv()
        remote(got_b, got_b, fl_send.at[s], fr_recv.at[s], left).wait_recv()

    grows = CORES * 2 * share
    blk = rows // n

    def group_rows(j):
        return pl.ds(pl.multiple_of(j * grows, grows), grows)

    def gate_mids(froms):
        return [remote(mgu.at[group_rows(j)], mgu.at[group_rows(j)], g_send.at[k], g_recv.at[k], to)
                for k, (j, to) in enumerate(zip(froms, (right, left, across)))]

    def exports():
        return [local(hb, h_out, e_sem.at[0]),
                local(xb.at[pl.ds(pl.multiple_of(chip * blk, blk), blk)], x1_out, e_sem.at[1])]

    def first_out():
        stage = OutStage(n, scale, rank, share, x, gain_mlp, (wo, wo_p, wo_f, wo_x), (wide, wide_f, wide_x),
                         (agu, agu_oth), (wob, attv, xb, mido, aob, bob, agub), wo_sem, lo_sem)
        wo_ready()
        gathered(0)
        loads = [local(att.at[0, j], attv.at[:, pl.ds(j * width, width)], att_sem.at[j]) for j in range(n)]
        loads += [local(x.at[first], xb, xo_sem)] + stage.lora(0, 0)
        for c in loads:
            c.start()
        for k in range(PAIR):
            stage.wo_start(k)
        for c in loads:
            c.wait()
        stage.first_product(0)
        stage.tiles(0, 0, stage.tiles_n, False)
        stage.norm(0, hb, mgu.at[group_rows(chip)])
        for c in gate_mids((chip, chip, chip)) + exports():
            c.start()

    def body(s, carry):
        g, slot = nseq + s, even(s)

        @pl.when(s + 1 < nseq)
        def _():
            x_copy(g + 1).start()
            for c in b_copies(s + 1):
                c.start()

        x_copy(g).wait()
        rms_rows(xbuf.at[even(g)], hbuf, gain, rows, 32)
        for c in mid_copies(s, (before, after, opposite)):
            c.wait_recv()
        mid = dot(sel[...], mids[s]).T.astype(BF16)
        for c in b_copies(s):
            c.wait()
        for p in range(3):
            z = dot_nt(hbuf[...], wbuf[pl.ds(p * width, width), :])
            z = z + scale * dot(mid, bbuf[slot, p])
            qkv[:, pl.ds(p * width, width)] = z.astype(BF16)

        @pl.when((s >= 2) & (s - 2 < keep))
        def _():
            out_right(s - 2).wait_send()
            out_left(s - 2).wait_send()

        @pl.when(s >= 2)
        def _():
            out_own(s - 2).wait()

        attend(qkv, attb.at[slot], width, group, dim, rows // 2)
        out_own(s).start()

        @pl.when(s < keep)
        def _():
            out_right(s).start()
            out_left(s).start()

        @pl.when(s == 0)
        def _():
            for k in range(2):
                pack_pass(k)


        @pl.when((s >= lag) & (s - lag < keep))
        def _():
            forward(s - lag)

        @pl.when(s == nseq - 2)
        def _():
            for k in range(2):
                pack_across(k)

        return carry

    loop(nseq, body, 0)

    def tail(s, carry):
        forward(s)
        return carry

    lax.fori_loop(max(min(nseq - lag, keep), 0), keep, tail, 0)
    first_out()
    for s in (nseq - 2, nseq - 1):
        if s < keep:
            out_right(s).wait_send()
            out_left(s).wait_send()
        out_own(s).wait()

    def finish(s, carry):
        pass_right(s).wait_send()
        pass_left(s).wait_send()

        @pl.when(s >= 1)
        def _():
            gathered(s)

        return carry

    loop(keep, finish, 0)

    def finish_mids(s, carry):
        for c in mid_copies(s):
            c.wait_send()
        return carry

    loop(nseq, finish_mids, 0)
    pack_end()
    for c in far[:4]:
        c.wait()
    far[4].wait_send()
    for c in gate_mids((before, after, opposite)):
        c.wait_recv()
    last = local(mgu, mg_out, e_sem.at[2])
    last.start()
    for c in gate_mids((chip, chip, chip)):
        c.wait_send()
    for c in exports() + [last]:
        c.wait()


def call_a(n, keep, scale, group, dim, share, x, gain, gain_mlp, wq, wk, wv, ar, agu, bqkv, wide, wo, wo_p, wg, wu, wd, lml):
    nseq, rows, model = x.shape[0] // CORES, x.shape[1], x.shape[2]
    own = wq.shape[0]
    width = own * CORES
    rank3 = bqkv.shape[1]
    crows = CORES * ar.shape[1]
    hbm = pl.BlockSpec(memory_space=pl.ANY)
    vmem = pl.BlockSpec(memory_space=pltpu.VMEM)
    dma = pltpu.SemaphoreType.DMA
    lag = min(5, nseq)
    flops = 2 * nseq * rows * model * (3 * width + rank3)
    return pl.pallas_call(
        functools.partial(kernel_a, n, lag, keep, scale, group, dim, share),
        out_shape=[
            jax.ShapeDtypeStruct((nseq, n, rows, width), BF16),
            jax.ShapeDtypeStruct((nseq, *ar.shape[1:]), BF16),
            jax.ShapeDtypeStruct((nseq, *agu.shape[1:]), BF16),
            jax.ShapeDtypeStruct((nseq, *bqkv.shape[1:]), BF16),
            jax.ShapeDtypeStruct((n - 1, *wide.shape), BF16),
            jax.ShapeDtypeStruct((n, nseq, *wide.shape[1:]), BF16),
            jax.ShapeDtypeStruct((n - 1, *wo.shape), BF16),
            jax.ShapeDtypeStruct((n, *wo.shape), BF16),
            jax.ShapeDtypeStruct(wg.shape, BF16),
            jax.ShapeDtypeStruct(wu.shape, BF16),
            jax.ShapeDtypeStruct(wd.shape, BF16),
            jax.ShapeDtypeStruct((nseq, *lml.shape[1:]), BF16),
            jax.ShapeDtypeStruct((rows, model), BF16),
            jax.ShapeDtypeStruct((rows // n, model), BF16),
            jax.ShapeDtypeStruct((n * CORES * 2 * share, rows), BF16),
        ],
        in_specs=[hbm, vmem, vmem] + [hbm] * 13,
        out_specs=[hbm] * 15,
        scratch_shapes=[
            pltpu.VMEM((3 * width, model), BF16),
            pltpu.VMEM((PAIR, rows, model), BF16),
            pltpu.VMEM((rows, model), BF16),
            pltpu.VMEM((PAIR, crows, model), BF16),
            pltpu.VMEM((PAIR, 3, rank3, width), BF16),
            pltpu.VMEM((rows, 3 * width), BF16),
            pltpu.VMEM((PAIR, rows, width), BF16),
            pltpu.VMEM((nseq, n * crows, rows), BF16),
            pltpu.VMEM((rank3, n * crows), BF16),
            pltpu.VMEM((PAIR, model, 512), BF16),
            pltpu.VMEM((rows, model), BF16),
            pltpu.VMEM((rows, model), BF16),
            pltpu.VMEM((rows, model), BF16),
            pltpu.VMEM((rows, rank3 // 3), BF16),
            pltpu.VMEM((1, rank3 // 3, model), BF16),
            pltpu.VMEM((1, rank3 // 3, model), BF16),
            pltpu.VMEM((1, CORES * 2 * share, model), BF16),
            pltpu.VMEM((n * CORES * 2 * share, rows), BF16),
            dma((TRIPLE,)), dma((PAIR,)), dma((PAIR, 2)), dma((PAIR, 3)), dma((PAIR, 3)), dma((5,)), dma((5,)), dma((5,)), dma((5,)),
            dma((TRIPLE, nseq)), dma((TRIPLE, nseq)),
        ] + [dma((PAIR,))] * 8 + [dma((10,))] * 2 + [
            dma((PAIR,)), dma((PAIR,)), dma((PAIR,)), dma((nseq,)), dma((nseq,)), dma((nseq,)), dma((nseq,)), dma((nseq,)), dma((nseq,)),
            dma((PAIR, CORES * n + 2)), dma((1, 3, CORES * n)), dma((n,)), dma, dma((TRIPLE,)), dma((TRIPLE,)), dma((TRIPLE,)),
        ],
        compiler_params=pltpu.CompilerParams(collective_id=0, has_side_effects=True, vmem_limit_bytes=VMEM_LIMIT),
        cost_estimate=pl.CostEstimate(flops=flops, bytes_accessed=3 * x.size, transcendentals=nseq * rows * rows * width // dim),
        name="qkv_attention",
    )(x, gain, gain_mlp, wq, wk, wv, ar, agu, bqkv, wide, wo, wo_p, wg, wu, wd, lml)


def kernel_b(n, keep, scale, rank, share,
             x, gain, att, wo, wo_p, wo_f, wo_x, wide, wide_f, wide_x, agu, agu_oth, wg, wg_o, wu, wu_o, wd, wd_o, lml, lml_o,
             h_first, x1_first, mg_first,
             y, att_t,
             wob, gub, wdb, attv, xb, hb, mb, zb, zm, x1b, yb, in1l, in1r, in2l, in2r, in1m, in2ml, in2mr, mgu, aob, bob, agub, lgb, lub, adb, bdb, sel, mido, midg,
             wo_sem, gu_sem, wd_sem, att_sem, x_sem, lo_sem, lg_sem, bd_sem,
             s1r, s1l, s2r, s2l, ar, al, yown, fr, fl, r1l, r1r, r2l, r2r, gl, gr, hl, hr, dsend, drecv,
             t_rs, t_ls, t_rl, t_rr, t_frs, t_fls, t_fl, t_fr,
             z1s, z1r, z2rs, z2rr, z2ls, z2lr, m_send, m_recv, e_sem):
    core, chip, right, left, partner = ring(n)
    nseq, rows, model = att.shape[0], x.shape[1], x.shape[2]
    width = att.shape[3]
    ff = wg.shape[1]
    first = core * nseq
    late = nseq - keep
    crows = CORES * 2 * share
    blk = rows // n
    half = blk // 2
    before, after, opposite = lax.rem(chip + n - 1, n), lax.rem(chip + 1, n), lax.rem(chip + 2, n)
    beyond = opposite * CORES + core
    wo_t, gu_t, wd_t = wob.shape[2], gub.shape[3], wdb.shape[2]
    wo_n, gu_n, wd_n = model // wo_t, ff // gu_t, model // wd_t
    greet(right, left, partner, beyond)

    stage = OutStage(n, scale, rank, share, x, gain, (wo, wo_p, wo_f, wo_x), (wide, wide_f, wide_x), (agu, agu_oth),
                     (wob, attv, xb, mido, aob, bob, agub), wo_sem, lo_sem)

    def gu_copies(k, own):
        at = pl.ds(pl.multiple_of(lax.rem(k, gu_n) * gu_t, gu_t), gu_t)
        slot = even(k)
        pair = (wg, wu) if own else (wg_o, wu_o)
        return [local(w.at[:, at], gub.at[slot, j], gu_sem.at[slot, j]) for j, w in enumerate(pair)]

    def gu_start(k):
        @pl.when(k < gu_n)
        def _():
            for c in gu_copies(k, True):
                c.start()

        @pl.when(k >= gu_n)
        def _():
            for c in gu_copies(k, False):
                c.start()

    def wd_copies(k):
        at = pl.ds(pl.multiple_of(k * wd_t, wd_t), wd_t)
        slot = even(k)
        return [local(w.at[:, at], wdb.at[slot, pl.ds(j * ff, ff)], wd_sem.at[slot, j]) for j, w in enumerate((wd, wd_o))]

    def att_copies(s):
        return [local(att.at[s, j], attv.at[:, pl.ds(j * width, width)], att_sem.at[j]) for j in range(n)]

    def att_start(s):
        @pl.when(s < keep)
        def _():
            start(att_copies(s))

        @pl.when(s >= keep)
        def _():
            k = jnp.maximum(s - keep, 0)
            late_in(k)
            for j, own in enumerate(att_copies(s)):
                @pl.when(chip == j)
                def _(own=own):
                    own.start()

                @pl.when(chip != j)
                def _(j=j):
                    local(att_t.at[k, j], attv.at[:, pl.ds(j * width, width)], att_sem.at[j]).start()

    def late_right(k):
        return remote(att.at[keep + k, chip], att_t.at[k, chip], t_rs.at[k], t_rl.at[k], right)

    def late_left(k):
        return remote(att.at[keep + k, chip], att_t.at[k, chip], t_ls.at[k], t_rr.at[k], left)

    def late_hops(k):
        a, b = att_t.at[k, before, head(rows // 2)], att_t.at[k, after, pl.ds(rows // 2, rows // 2)]
        return remote(a, a, t_frs.at[k], t_fl.at[k], right), remote(b, b, t_fls.at[k], t_fr.at[k], left)

    def late_pass(k):
        hop_r, hop_l = late_hops(k)
        remote(att.at[keep + k, chip], att_t.at[k, before], t_rs.at[k], t_rl.at[k], right).wait_recv()
        hop_r.start()
        remote(att.at[keep + k, chip], att_t.at[k, after], t_ls.at[k], t_rr.at[k], left).wait_recv()
        hop_l.start()

    def late_in(k):
        a, b = att_t.at[k, opposite, head(rows // 2)], att_t.at[k, opposite, pl.ds(rows // 2, rows // 2)]
        remote(a, a, t_frs.at[k], t_fl.at[k], right).wait_recv()
        remote(b, b, t_fls.at[k], t_fr.at[k], left).wait_recv()

    def x_copy(s):
        return local(x.at[first + s], xb, x_sem)

    def lora_o(s):
        return stage.lora(s, even(s))

    def lora_m(s):
        slot, out = even(s), []
        for j, (src, k) in enumerate(((lml, first + s), (lml_o, s))):
            at = pl.ds(j * ff, ff)
            out.append(local(src.at[k, head(rank)], lgb.at[slot, head(rank), at], lg_sem.at[slot, 3 * j]))
            out.append(local(src.at[k, pl.ds(rank, rank)], lub.at[slot, pl.ds(rank, rank), at], lg_sem.at[slot, 3 * j + 1]))
            out.append(local(src.at[k, pl.ds(2 * rank, rank)], adb.at[slot, head(rank), at], lg_sem.at[slot, 3 * j + 2]))
        return out

    def start(copies):
        for c in copies:
            c.start()

    def wait(copies):
        for c in copies:
            c.wait()

    def rows_of(j, size=blk, shift=0):
        return pl.ds(pl.multiple_of(j * blk + shift, size), size)

    def rs1_right(s):
        return remote(zb.at[third(s), rows_of(opposite, half)], in1l.at[third(s)], s1r.at[s], r1l.at[s], right)

    def rs1_left(s):
        return remote(zb.at[third(s), rows_of(opposite, half, half)], in1r.at[third(s)], s1l.at[s], r1r.at[s], left)

    def rs2_right(s):
        return remote(zb.at[third(s), rows_of(after)], in2l.at[third(s)], s2r.at[s], r2l.at[s], right)

    def rs2_left(s):
        return remote(zb.at[third(s), rows_of(before)], in2r.at[third(s)], s2l.at[s], r2r.at[s], left)

    def ag1_right(s):
        return remote(yb.at[even(s)], y.at[first + s, rows_of(chip)], ar.at[s], gl.at[s], right)

    def ag1_left(s):
        return remote(yb.at[even(s)], y.at[first + s, rows_of(chip)], al.at[s], gr.at[s], left)

    def ag1_own(s):
        return local(yb.at[even(s)], y.at[first + s, rows_of(chip)], yown.at[s])

    def ag2_right(s, block):
        part = y.at[first + s, rows_of(block, half)]
        return remote(part, part, fr.at[s], hl.at[s], right)

    def ag2_left(s, block):
        part = y.at[first + s, rows_of(block, half, half)]
        return remote(part, part, fl.at[s], hr.at[s], left)

    def across(s, k, block):
        part = y.at[first + s, rows_of(block)]
        return remote(yb.at[even(s)] if k == 0 else part, part, dsend.at[k, s], drecv.at[k, s], partner)

    def across_in(s, k):
        there = y.at[(1 - core) * nseq + s, rows_of((chip, before, after, opposite)[k])]
        return remote(there, there, dsend.at[k, s], drecv.at[k, s], partner)

    def lanes_of(j):
        return pl.ds(pl.multiple_of(j * blk, blk), blk)

    def zm1(s):
        return remote(zm.at[third(s), :, lanes_of(opposite)], in1m.at[third(s)], z1s.at[s], z1r.at[s], right)

    def zm2_right(s):
        return remote(zm.at[third(s), :, lanes_of(after)], in2ml.at[third(s)], z2rs.at[s], z2rr.at[s], right)

    def zm2_left(s):
        return remote(zm.at[third(s), :, lanes_of(before)], in2mr.at[third(s)], z2ls.at[s], z2lr.at[s], left)

    def rank_rows(j):
        return pl.ds(pl.multiple_of(j * crows, crows), crows)

    def mid_copies(s, froms):
        return [remote(mgu.at[s, rank_rows(j)], mgu.at[s, rank_rows(j)], m_send.at[k, s], m_recv.at[k, s], to)
                for k, (j, to) in enumerate(zip(froms, (right, left, beyond)))]

    def do_rs2(s):
        slot = third(s)
        zm1(s).wait_recv()
        at = lanes_of(after)
        zm[slot, :, at] = (zm[slot, :, at].astype(F32) + in1m[slot].astype(F32)).astype(BF16)
        zm2_right(s).start()
        zm2_left(s).start()
        rs1_right(s).wait_recv()
        at = rows_of(after, half)
        zb[slot, at, :] = (zb[slot, at, :].astype(F32) + in1l[slot].astype(F32)).astype(BF16)
        rs2_right(s).start()
        rs1_left(s).wait_recv()
        at = rows_of(before, half, half)
        zb[slot, at, :] = (zb[slot, at, :].astype(F32) + in1r[slot].astype(F32)).astype(BF16)
        rs2_left(s).start()

    def do_rs3(s):
        slot, yslot = third(s), even(s)

        @pl.when(s >= 2)
        def _():
            ag1_right(s - 2).wait_send()
            ag1_left(s - 2).wait_send()
            ag1_own(s - 2).wait()
            across(s - 2, 0, chip).wait_send()

        rs2_right(s).wait_recv()
        rs2_left(s).wait_recv()
        mine = zb.at[slot, rows_of(chip)]
        zm2_right(s).wait_recv()
        zm2_left(s).wait_recv()
        mid = zm[slot, :, lanes_of(chip)].astype(F32) + in2ml[slot].astype(F32) + in2mr[slot].astype(F32)
        mid = mid.T.astype(BF16)

        def piece(k, carry):
            at = pl.ds(pl.multiple_of(k * wo_t, wo_t), wo_t)
            z = mine[:, at].astype(F32) + in2l[slot, :, at].astype(F32) + in2r[slot, :, at].astype(F32)
            z = z + scale * dot(mid, bdb[s, :, at])
            yb[yslot, :, at] = (x1b[lax.rem(s, 4), :, at].astype(F32) + z).astype(BF16)
            return carry

        loop(wo_n, piece, 0)
        ag1_right(s).start()
        ag1_left(s).start()
        ag1_own(s).start()
        across(s, 0, chip).start()

    def do_ag2(s):
        remote(yb.at[0], y.at[first + s, rows_of(before)], ar.at[s], gl.at[s], right).wait_recv()
        ag2_right(s, before).start()
        across(s, 1, before).start()
        remote(yb.at[0], y.at[first + s, rows_of(after)], al.at[s], gr.at[s], left).wait_recv()
        ag2_left(s, after).start()
        across(s, 2, after).start()

    def do_across(s):
        ag2_right(s, opposite).wait_recv()
        ag2_left(s, opposite).wait_recv()
        across(s, 3, opposite).start()

    def when(cond, f, s):
        @pl.when(cond)
        def _():
            f(s)

    for k in range(min(late, 2)):
        late_right(k).start()
        late_left(k).start()
    bd_copies = [local(stage.share_of((wide, wide_f, wide_x), cross, j).at[pl.ds(0 if cross else first, nseq), pl.ds(2 * rank, rank)],
                       bdb.at[:, :, stage.cols(d)], bd_sem.at[4 * cross + j]) for d, cross, j in stage.shares]
    done = [local(h_first, hb.at[0], e_sem.at[0]), local(x1_first, x1b.at[0], e_sem.at[1]), local(mg_first, mgu.at[0], e_sem.at[2])]
    start(done)
    start(bd_copies)
    sel[...] = pick(sel.shape, share, rank, 2, 1)
    for k in range(2):
        stage.wo_start(k)
        start(gu_copies(k, True))
        start(wd_copies(k))
    att_start(jnp.int32(1))
    x_copy(1).start()
    start(lora_o(1))
    lgb[...] = jnp.zeros_like(lgb)
    lub[...] = jnp.zeros_like(lub)
    start(lora_m(0))
    wait(bd_copies)
    wait(done)

    def out_proj(s):
        slot = even(s)
        wait(lora_o(s))
        wait(att_copies(s))
        x_copy(s).wait()
        stage.first_product(slot)
        stage.tiles(slot, 0, wo_n // 2, s + 1 < nseq)

    def out_proj_end(s):
        slot = even(s)
        stage.tiles(slot, wo_n // 2, wo_n, s + 1 < nseq)
        stage.norm(slot, hb.at[slot], mgu.at[s, rank_rows(chip)])
        start(mid_copies(s, (chip, chip, chip)))
        for k in range(2, late):
            @pl.when(s == k - 1)
            def _(k=k):
                late_right(k).start()
                late_left(k).start()

        x1b[lax.rem(s, 4)] = xb[rows_of(chip), :]

        @pl.when(s + 1 < nseq)
        def _():
            start(lora_o(s + 1))
            att_start(s + 1)
            x_copy(s + 1).start()

    def gate_up(s):
        slot = even(s)
        @pl.when(s >= 1)
        def _():
            for c in mid_copies(s, (before, after, opposite)):
                c.wait_recv()

        midg[...] = dot(sel[...], mgu[s]).T.astype(BF16)
        wait(lora_m(s))
        gate_tiles(s, 0, gu_n)

    def gate_tiles(s, lo, hi):
        slot = even(s)
        h = hb.at[slot]
        mid = midg[...]

        def tile(k, carry):
            at = pl.ds(pl.multiple_of(k * gu_t, gu_t), gu_t)
            wait(gu_copies(k, True))
            g = dot(h[...], gub[even(k), 0]) + scale * dot(mid, lgb[slot, :, at])
            u = dot(h[...], gub[even(k), 1]) + scale * dot(mid, lub[slot, :, at])
            g = g.astype(BF16).astype(F32)
            u = u.astype(BF16).astype(F32)
            mb[:, at] = (jax.nn.silu(g) * u).astype(BF16)

            @pl.when((k + 2 < 2 * gu_n) | (s + 1 < nseq))
            def _():
                gu_start(lax.rem(k + 2, 2 * gu_n))

            return carry

        lax.fori_loop(lo, hi, tile, 0)

    def gate_up_end(s):
        gate_tiles(s, gu_n, 2 * gu_n)

        @pl.when(s + 1 < nseq)
        def _():
            start(lora_m(s + 1))

    def down(s):
        slot = third(s)

        @pl.when(s >= 3)
        def _():
            rs1_right(s - 3).wait_send()
            rs1_left(s - 3).wait_send()
            rs2_right(s - 3).wait_send()
            rs2_left(s - 3).wait_send()
            zm1(s - 3).wait_send()
            zm2_right(s - 3).wait_send()
            zm2_left(s - 3).wait_send()

        zm[slot] = dot_nt(adb[even(s)], mb[...]).astype(BF16)

        def tile(k, carry):
            at = pl.ds(pl.multiple_of(k * wd_t, wd_t), wd_t)
            wait(wd_copies(k))
            zb[slot, :, at] = dot(mb[...], wdb[even(k)]).astype(BF16)

            @pl.when((k + 2 < wd_n) | (s + 1 < nseq))
            def _():
                start(wd_copies(lax.rem(k + 2, wd_n)))

            return carry

        loop(wd_n, tile, 0)
        zm1(s).start()
        rs1_right(s).start()
        rs1_left(s).start()

    def step(f, t, lag, ahead=0):
        s = t - lag + ahead
        when((s >= 0) & (s < nseq), f, s)

    def body(t, carry):
        step(out_proj, t, 0, 1)
        step(do_rs3, t, 2)
        step(out_proj_end, t, 0, 1)
        for k, stages in enumerate(((), (gate_up, do_rs2, do_ag2, gate_up_end), (down,))):
            for f in stages:
                step(f, t, {do_rs2: 1, do_ag2: 2}.get(f, 0))
            if k < late:
                when(t == 0, lambda _, k=k: late_pass(k), t)
        step(do_across, t, 3)
        return carry

    loop(nseq + 3, body, 0)

    for s in range(max(nseq - 3, 0), nseq):
        rs1_right(s).wait_send()
        rs1_left(s).wait_send()
        rs2_right(s).wait_send()
        rs2_left(s).wait_send()
        zm1(s).wait_send()
        zm2_right(s).wait_send()
        zm2_left(s).wait_send()
    for s in range(max(nseq - 2, 0), nseq):
        ag1_right(s).wait_send()
        ag1_left(s).wait_send()
        ag1_own(s).wait()
        across(s, 0, chip).wait_send()

    def finish(s, carry):
        @pl.when(s >= 1)
        def _():
            for c in mid_copies(s, (chip, chip, chip)):
                c.wait_send()

        ag2_right(s, before).wait_send()
        ag2_left(s, after).wait_send()
        for k, block in ((1, before), (2, after), (3, opposite)):
            across(s, k, block).wait_send()
        for k in range(4):
            across_in(s, k).wait_recv()
        return carry

    loop(nseq, finish, 0)
    for k in range(late):
        late_right(k).wait_send()
        late_left(k).wait_send()
        for hop in late_hops(k):
            hop.wait_send()


def call_b(n, keep, scale, rank, share, x, gain, att, wo, wo_p, wo_f, wo_x, wide, wide_f, wide_x, agu, agu_oth, wg, wg_o, wu, wu_o, wd, wd_o, lml, lml_o, h_first, x1_first, mg_first):
    nseq, rows, model, ff = att.shape[0], x.shape[1], x.shape[2], wg.shape[1]
    hbm = pl.BlockSpec(memory_space=pl.ANY)
    vmem = pl.BlockSpec(memory_space=pltpu.VMEM)
    dma = pltpu.SemaphoreType.DMA
    blk = rows // n
    ndev = CORES * n
    tile = 512
    flops = 2 * nseq * rows * (model * model + 3 * model * ff * CORES)
    return pl.pallas_call(
        functools.partial(kernel_b, n, keep, scale, rank, share),
        out_shape=[jax.ShapeDtypeStruct(x.shape, BF16), jax.ShapeDtypeStruct((nseq - keep, *att.shape[1:]), BF16)],
        in_specs=[hbm, vmem] + [hbm] * 21,
        out_specs=[hbm] * 2,
        scratch_shapes=[
            pltpu.VMEM((PAIR, model, tile), BF16),
            pltpu.VMEM((PAIR, 2, model, tile // 2), BF16),
            pltpu.VMEM((PAIR, CORES * ff, tile), BF16),
            pltpu.VMEM((rows, model), BF16),
            pltpu.VMEM((rows, model), BF16),
            pltpu.VMEM((PAIR, rows, model), BF16),
            pltpu.VMEM((rows, CORES * ff), BF16),
            pltpu.VMEM((TRIPLE, rows, model), BF16),
            pltpu.VMEM((TRIPLE, rank, rows), BF16),
            pltpu.VMEM((QUAD, blk, model), BF16),
            pltpu.VMEM((PAIR, blk, model), BF16),
            pltpu.VMEM((TRIPLE, blk // 2, model), BF16),
            pltpu.VMEM((TRIPLE, blk // 2, model), BF16),
            pltpu.VMEM((TRIPLE, blk, model), BF16),
            pltpu.VMEM((TRIPLE, blk, model), BF16),
            pltpu.VMEM((TRIPLE, rank, blk), BF16),
            pltpu.VMEM((TRIPLE, rank, blk), BF16),
            pltpu.VMEM((TRIPLE, rank, blk), BF16),
            pltpu.VMEM((nseq, n * CORES * 2 * share, rows), BF16),
            pltpu.VMEM((PAIR, rank, model), BF16),
            pltpu.VMEM((PAIR, rank, model), BF16),
            pltpu.VMEM((PAIR, CORES * 2 * share, model), BF16),
            pltpu.VMEM((PAIR, 2 * rank, CORES * ff), BF16),
            pltpu.VMEM((PAIR, 2 * rank, CORES * ff), BF16),
            pltpu.VMEM((PAIR, rank, CORES * ff), BF16),
            pltpu.VMEM((nseq, rank, model), BF16),
            pltpu.VMEM((2 * rank, 2 * rank), BF16),
            pltpu.VMEM((rows, rank), BF16),
            pltpu.VMEM((rows, 2 * rank), BF16),
            dma((PAIR, ndev + 2)), dma((PAIR, 2)), dma((PAIR, 2)), dma((n,)), dma, dma((PAIR, 3, ndev)), dma((PAIR, 6)), dma((ndev,)),
        ] + [dma((nseq,))] * 17 + [dma((QUAD, nseq))] * 2 + [dma((nseq - keep,))] * 8 + [dma((nseq,))] * 6 + [dma((TRIPLE, nseq))] * 2 + [dma((TRIPLE,))],
        compiler_params=pltpu.CompilerParams(collective_id=1, has_side_effects=True, vmem_limit_bytes=VMEM_LIMIT),
        cost_estimate=pl.CostEstimate(flops=flops, bytes_accessed=4 * x.size, transcendentals=0),
        name="out_mlp",
    )(x, gain, att, wo, wo_p, wo_f, wo_x, wide, wide_f, wide_x, agu, agu_oth, wg, wg_o, wu, wu_o, wd, wd_o, lml, lml_o, h_first, x1_first, mg_first)[0]


def solution(mesh):
    n = mesh.shape["tp"] // CORES
    act_spec = P("dp", N, N)
    w_head, w_out, w_col, w_row = P(N, "tp", N), P("tp", N, N), P(N, "tp"), P("tp", N)
    a_rank, b_head, b_col = P(N, N, "tp"), P(N, N, "tp", N), P(N, N, "tp")
    a_head, a_row = P(N, "tp", N, N), P(N, "tp", N)
    in_specs = (act_spec, P("dp"), P(N), P(N), w_head, w_head, w_head, w_out, w_col, w_col, w_row,
                a_rank, b_head, a_rank, b_head, a_rank, b_head, a_head, b_col, a_rank, b_col, a_rank, b_col, a_row, b_col)

    def local_layer(x_in, adapter_ids, gain_attn, gain_mlp, w_q, w_k, w_v, w_o, w_gate, w_up, w_down,
                    a_q, b_q, a_k, b_k, a_v, b_v, a_o, b_o, a_gate, b_gate, a_up, b_up, a_down, b_down):
        nseq, model = x_in.shape[0], x_in.shape[2]
        rank, dim = b_q.shape[1], w_q.shape[2]
        own = w_q.shape[1] * dim
        scale = LORA_ALPHA / rank
        share = a_q.shape[2]
        group = math.lcm(dim, 128) // dim
        keep = max(nseq // CORES - 3, 1)

        def take(*stacks):
            return jnp.take(jnp.concatenate(stacks, axis=1), adapter_ids, axis=0, mode="clip")

        def turn(stack):
            return jnp.swapaxes(stack, 1, 2)

        wo = w_o.reshape(own, model)
        ndev = n * CORES
        turns = [(d, (d + CORES * (1 if d % CORES == 0 else -1)) % ndev) for d in range(ndev)]
        wo_p = lax.ppermute(wo, "tp", turns)
        ar = take(turn(a_q), turn(a_k), turn(a_v), jnp.zeros((a_q.shape[0], share, model), BF16))
        agu = take(turn(a_gate), turn(a_up))
        bqkv = take(*[b.reshape(-1, rank, own) for b in (b_q, b_k, b_v)])
        wide = take(turn(a_o.reshape(-1, own, rank)), b_o, b_down)
        lml = take(b_gate, b_up, turn(a_down))
        flat = [jnp.transpose(w, (1, 2, 0)).reshape(own, model) for w in (w_q, w_k, w_v)]
        att, _, agu_oth, _, wide_f, wide_x, wo_f, wo_x, wg_o, wu_o, wd_o, lml_o, *head = call_a(
            n, keep, scale, group, dim, share, x_in, gain_attn.reshape(1, model), gain_mlp.reshape(1, model), *flat, ar, agu, bqkv, wide,
            wo, wo_p, w_gate, w_up, w_down, lml)
        return call_b(n, keep, scale, rank, share, x_in, gain_mlp.reshape(1, model), att, wo, wo_p, wo_f, wo_x, wide, wide_f, wide_x,
                      agu, agu_oth, w_gate, wg_o, w_up, wu_o, w_down, wd_o, lml, lml_o, *head)

    return jax.shard_map(local_layer, mesh=mesh, in_specs=in_specs, out_specs=act_spec, check_vma=False)
```
